8 devices in a mesh: col: 2 (over z, y), row: 4 (over x, core).
Axes of the slice: x: 2, y: 2, z: 1, core: 2. Of those that a mesh axis runs over, the one named last changes fastest.
Arguments:
- w_gate: float32 [1024, 2816], P('row', 'col')
- w_up: float32 [1024, 2816], P('row', 'col')
- w_down: float32 [2816, 1024], P('row', 'col')
- x_norm: bfloat16 [2048, 1024], P(None, 'row')
- x_act: bfloat16 [2048, 2816], P(None, 'row')
- dy_gate: bfloat16 [2048, 2816], P(None, 'col')
- dy_up: bfloat16 [2048, 2816], P(None, 'col')
- dy_down: bfloat16 [2048, 1024], P(None, 'col')
- r_gate: float32 [1024], P('row')
- c_gate: float32 [2816], P('col')
- r_up: float32 [1024], P('row')
- c_up: float32 [2816], P('col')
- r_down: float32 [2816], P('row')
- c_down: float32 [1024], P('col')
- hyper_params: float32 [3], replicated
Outputs:
- output 1: float32 [1024, 2816], P('row', 'col')
- output 2: float32 [1024, 2816], P('row', 'col')
- output 3: float32 [2816, 1024], P('row', 'col')
- output 4: float32 [1024], P('row')
- output 5: float32 [2816], P('col')
- output 6: float32 [1024], P('row')
- output 7: float32 [2816], P('col')
- output 8: float32 [2816], P('row')
- output 9: float32 [1024], P('col')
- output 10: bfloat16 [2048, 1024], P(None, 'row')
- output 11: bfloat16 [2048, 2816], P(None, 'row')
All inputs are finite; a program needn't handle non-finite values.
Results may differ from the reference program's by a relative error of at most 0.001.
Values are sent between devices in bfloat16 or wider.
A program may use at most 1 GiB of HBM per device.

```python
import jax
import jax.numpy as jnp
from jax import lax

D_MODEL = 1024
D_FF = 2816
TOKENS = 2048
EPS_ONE = 1e-30
EPS_TWO = 1e-3
TWO_PI = 6.283185307179586


def smooth_field(key, length, log_scale):
    key_amp, key_phase = jax.random.split(key)
    ampl_k = jax.random.normal(key_amp, (3,), jnp.float32)
    phase_k = jax.random.uniform(key_phase, (3,), jnp.float32, minval=0.0, maxval=TWO_PI)
    position = jnp.arange(length, dtype=jnp.float32) / length
    freq_k = jnp.arange(1, 4, dtype=jnp.float32)
    waves = jnp.cos(TWO_PI * position[:, None] * freq_k[None, :] + phase_k[None, :])
    return jnp.exp(log_scale * jnp.sum(waves * ampl_k[None, :], axis=1) / 1.7)


def draw_weight(key, rows, cols):
    key_z, key_r, key_c = jax.random.split(key, 3)
    noise = jax.random.normal(key_z, (rows, cols), jnp.float32)
    row_prof = smooth_field(key_r, rows, 0.5)
    col_prof = smooth_field(key_c, cols, 0.5)
    return noise * (rows ** -0.5) * row_prof[:, None] * col_prof[None, :]


def draw_tokens(key, cols, scale):
    key_z, key_a, key_b = jax.random.split(key, 3)
    noise = jax.random.normal(key_z, (TOKENS, cols), jnp.float32)
    first_half = (jnp.arange(TOKENS) < TOKENS // 2)[:, None]
    profile = jnp.where(first_half, smooth_field(key_a, cols, 0.8)[None, :], smooth_field(key_b, cols, 0.8)[None, :])
    return (noise * profile * scale).astype(jnp.bfloat16)


def draw_stat(key, length):
    return jax.random.uniform(key, (length,), jnp.float32, minval=0.5, maxval=3.0)


def setup_inputs(seed: int = 0) -> dict:
    keys = jax.random.split(jax.random.key(seed), 15)
    tok_scale = TOKENS ** -0.5
    low_end = jnp.array([0.6, 0.6, 0.15], dtype=jnp.float32)
    span_len = jnp.array([0.25, 0.6, 0.15], dtype=jnp.float32)
    unit_draw = jax.random.uniform(keys[14], (3,), jnp.float32)
    return {
        'w_gate': draw_weight(keys[0], D_MODEL, D_FF),
        'w_up': draw_weight(keys[1], D_MODEL, D_FF),
        'w_down': draw_weight(keys[2], D_FF, D_MODEL),
        'x_norm': draw_tokens(keys[3], D_MODEL, tok_scale),
        'x_act': draw_tokens(keys[4], D_FF, tok_scale),
        'dy_gate': draw_tokens(keys[5], D_FF, 1.0),
        'dy_up': draw_tokens(keys[6], D_FF, 1.0),
        'dy_down': draw_tokens(keys[7], D_MODEL, 1.0),
        'r_gate': draw_stat(keys[8], D_MODEL),
        'c_gate': draw_stat(keys[9], D_FF),
        'r_up': draw_stat(keys[10], D_MODEL),
        'c_up': draw_stat(keys[11], D_FF),
        'r_down': draw_stat(keys[12], D_FF),
        'c_down': draw_stat(keys[13], D_MODEL),
        'hyper_params': low_end + span_len * unit_draw,
    }


def factored_step(w_old, grad_w, r_old, c_old, hyper_params):
    beta_two = hyper_params[0]
    grad_sq = grad_w * grad_w + EPS_ONE
    r_new = beta_two * r_old + (1.0 - beta_two) * jnp.mean(grad_sq, axis=1)
    c_new = beta_two * c_old + (1.0 - beta_two) * jnp.mean(grad_sq, axis=0)
    v_est = r_new[:, None] * c_new[None, :] / jnp.mean(r_new)
    update = grad_w * lax.rsqrt(v_est)
    rms_u = jnp.sqrt(jnp.mean(update * update))
    update_hat = update / jnp.maximum(1.0, rms_u / hyper_params[2])
    step_size = hyper_params[1] * jnp.maximum(EPS_TWO, jnp.sqrt(jnp.mean(w_old * w_old)))
    return w_old - step_size * update_hat, r_new, c_new


def weight_grad(activations, grad_out):
    return jnp.dot(activations.T, grad_out, preferred_element_type=jnp.float32)


def input_grad(grad_out, weight):
    return jnp.dot(grad_out, weight.astype(jnp.bfloat16).T, preferred_element_type=jnp.float32)


def reference(w_gate, w_up, w_down, x_norm, x_act, dy_gate, dy_up, dy_down, r_gate, c_gate, r_up, c_up, r_down, c_down, hyper_params):
    new_gate, r_gate_new, c_gate_new = factored_step(w_gate, weight_grad(x_norm, dy_gate), r_gate, c_gate, hyper_params)
    new_up, r_up_new, c_up_new = factored_step(w_up, weight_grad(x_norm, dy_up), r_up, c_up, hyper_params)
    new_down, r_down_new, c_down_new = factored_step(w_down, weight_grad(x_act, dy_down), r_down, c_down, hyper_params)
    dx_norm = (input_grad(dy_gate, w_gate) + input_grad(dy_up, w_up)).astype(jnp.bfloat16)
    dx_act = input_grad(dy_down, w_down).astype(jnp.bfloat16)
    return (new_gate, new_up, new_down, r_gate_new, c_gate_new, r_up_new, c_up_new, r_down_new, c_down_new, dx_norm, dx_act)
```

```python
import functools

import jax
import jax.numpy as jnp
from jax import lax
from jax.experimental import pallas as pl
from jax.experimental.pallas import tpu as pltpu
from jax.sharding import PartitionSpec as P

EPS_ONE = 1e-30
EPS_TWO = 1e-3
MESH = pl.DeviceIdType.MESH
F32 = jnp.float32
BF16 = jnp.bfloat16
NT = (((1,), (1,)), ((), ()))
CHUNK = 256


def dot(a, b, dims=(((1,), (0,)), ((), ()))):
    return lax.dot_general(a, b, dims, preferred_element_type=F32)


def spans(total, step):
    return [(lo, min(step, total - lo)) for lo in range(0, total, step)]


def to_row(column):
    return jnp.transpose(jnp.broadcast_to(column, (column.shape[0], 128)))[0:1, :]


def to_columns(row):
    return jnp.transpose(jnp.broadcast_to(row, (128, row.shape[1])))


def exchange_kernel(
    m_total, wg, wu, wd, xn, xat, dyg, dyu, dyd, rg, cg, ru, cu, rd, cd, hp,
    gg_o, gu_o, gd_o, wd_o, dyd_o, half_o, rcg_o, rcu_o, rcd_o, rrow_o, crow_o, scal_o,
    wg_v, wu_v, wd_v, wgb, wub, wdb, dyg_v, dyu_v, dyd_v, xn_v, xnt, xat_v, g_g, g_u, g_d,
    p_send, p_recv, p_own, half_v, rs_send, rs_recv, cs_send, cs_recv, s2_send, s2_recv,
    in_sem, out_sem, bulk_send, bulk_recv, p_ssem, p_rsem, st_send, st_recv, s2_ssem, s2_rsem,
):
    c = lax.axis_index("col")
    r = lax.axis_index("row")
    rows = {0: r, 1: r + 1 - 2 * (r % 2), 2: (r + 2) % 4, 3: 3 - r}
    cols = {0: c, 1: 1 - c}
    peers = [(a, b) for a in (0, 1) for b in (0, 1, 2, 3) if (a, b) != (0, 0)]

    def peer(a, b):
        return (cols[a], rows[b])

    def remote(src, dst, ssem, rsem, who):
        return pltpu.make_async_remote_copy(
            src_ref=src, dst_ref=dst, send_sem=ssem, recv_sem=rsem, device_id=who, device_id_type=MESH
        )

    tokens = dyg.shape[0]
    half = tokens // 2
    quarter = tokens // 4
    steps = half // CHUNK
    mine, theirs = pl.multiple_of(c * half, half), pl.multiple_of((1 - c) * half, half)

    loads = []

    def load(src, dst):
        copy = pltpu.make_async_copy(src, dst, in_sem.at[len(loads)])
        copy.start()
        loads.append(copy)
        return copy

    l_wg = load(wg, wg_v)
    l_wu = load(wu, wu_v)
    l_dg1 = load(dyg.at[pl.ds(theirs, half)], dyg_v.at[pl.ds(theirs, half)])
    l_du1 = load(dyu.at[pl.ds(theirs, half)], dyu_v.at[pl.ds(theirs, half)])
    l_xn = load(xn, xn_v)
    l_dg2 = load(dyg.at[pl.ds(mine, half)], dyg_v.at[pl.ds(mine, half)])
    l_du2 = load(dyu.at[pl.ds(mine, half)], dyu_v.at[pl.ds(mine, half)])
    l_xat = load(xat, xat_v)
    l_dyd = load(dyd, dyd_v)
    l_wd = load(wd, wd_v)

    barrier = pltpu.get_barrier_semaphore()
    for a, b in peers:
        pl.semaphore_signal(barrier, inc=1, device_id=peer(a, b), device_id_type=MESH)
    pl.semaphore_wait(barrier, 7)

    my_rows = pl.ds(pl.multiple_of(r * quarter, quarter), quarter)
    f1 = remote(dyd.at[my_rows], dyd_o.at[c, my_rows], bulk_send.at[0], bulk_recv.at[0], peer(1, 0))
    f1.start()

    outs = []

    def store(src, dst):
        copy = pltpu.make_async_copy(src, dst, out_sem.at[len(outs)])
        copy.start()
        outs.append(copy)

    l_wg.wait()
    wgb[...] = wg_v[...].astype(BF16)
    l_wu.wait()
    wub[...] = wu_v[...].astype(BF16)
    l_dg1.wait()
    l_du1.wait()

    def p_copy(i):
        rows_i = pl.ds(pl.multiple_of(i * CHUNK, CHUNK), CHUNK)
        return remote(p_send.at[rows_i], p_recv.at[rows_i], p_ssem.at[i], p_rsem.at[i], peer(1, 0))

    def partial(base, i):
        rows_i = pl.ds(pl.multiple_of(base + i * CHUNK, CHUNK), CHUNK)
        return dot(dyg_v[rows_i, :], wgb[...], NT) + dot(dyu_v[rows_i, :], wub[...], NT)

    @pl.loop(0, steps)
    def _(i):
        p_send[pl.ds(pl.multiple_of(i * CHUNK, CHUNK), CHUNK), :] = partial(theirs, i)
        p_copy(i).start()

    rs_send[...] = jnp.zeros_like(rs_send)
    cs_send[...] = jnp.zeros_like(cs_send)
    l_xn.wait()
    for lo, width in spans(tokens, 256):
        xnt[:, lo:lo + width] = jnp.transpose(xn_v[lo:lo + width, :])
    l_dg2.wait()
    l_du2.wait()

    def gradient(index, lhs, rhs, out):
        m, n = out.shape
        acc = jnp.zeros((m, 128), F32)
        for lo, width in spans(n, 256):
            g = dot(lhs[...], rhs[:, lo:lo + width])
            out[:, lo:lo + width] = g
            sq = g * g + EPS_ONE
            cs_send[index:index + 1, lo:lo + width] = jnp.sum(sq, axis=0, keepdims=True)
            for part in range(0, width, 128):
                acc = acc + sq[:, part:part + 128]
        rs_send[index:index + 1, 0:m] = to_row(jnp.sum(acc, axis=1, keepdims=True))

    gradient(0, xnt, dyg_v, g_g)
    gradient(1, xnt, dyu_v, g_u)
    l_xat.wait()
    l_dyd.wait()
    gradient(2, xat_v, dyd_v, g_d)

    s1_row = remote(rs_send, rs_recv, st_send.at[0], st_recv.at[0], peer(1, 0))
    s1_row.start()
    s1_col = []
    for b in (1, 2, 3):
        copy = remote(cs_send, cs_recv.at[b - 1], st_send.at[b], st_recv.at[b], peer(0, b))
        copy.start()
        s1_col.append(copy)

    store(g_g, gg_o)
    store(g_u, gu_o)
    store(g_d, gd_o)
    store(dyd_v, dyd_o.at[c])

    l_wd.wait()
    wdb[...] = wd_v[...].astype(BF16)
    f3 = remote(wdb, wd_o.at[c], bulk_send.at[1], bulk_recv.at[1], peer(1, 0))
    f3.start()
    store(wdb, wd_o.at[c])

    w_sq = [jnp.sum(jnp.sum(w[...] * w[...], axis=0, keepdims=True), axis=1, keepdims=True) for w in (wg_v, wu_v, wd_v)]

    f1.wait_recv()
    shares = []
    for b in (1, 2, 3):
        copy = remote(dyd_o.at[1 - c, my_rows], dyd_o.at[1 - c, my_rows], bulk_send.at[1 + b], bulk_recv.at[1 + b], peer(0, b))
        copy.start()
        shares.append(copy)

    @pl.loop(0, steps)
    def _(i):
        p_own[pl.ds(pl.multiple_of(i * CHUNK, CHUNK), CHUNK), :] = partial(mine, i)

    s1_row.wait_recv()
    for copy in s1_col:
        copy.wait_recv()
    beta = hp[0]
    shapes = [g.shape for g in (g_g, g_u, g_d)]
    qs, ss = [], []
    for index, (g, r_ref, c_ref, rc_o) in enumerate(((g_g, rg, cg, rcg_o), (g_u, ru, cu, rcu_o), (g_d, rd, cd, rcd_o))):
        m, n = shapes[index]
        m_all, n_all = m * 4, n * 2
        row_sum = rs_send[index:index + 1, 0:m] + rs_recv[index:index + 1, 0:m]
        col_sum = (cs_send[index:index + 1, 0:n] + cs_recv[0, index:index + 1, 0:n]) + (
            cs_recv[1, index:index + 1, 0:n] + cs_recv[2, index:index + 1, 0:n])
        r_new = beta * r_ref[...].reshape(1, m) + (1.0 - beta) * (row_sum / n_all)
        c_new = beta * c_ref[...].reshape(1, n) + (1.0 - beta) * (col_sum / m_all)
        rrow_o[index:index + 1, 0:m] = r_new
        crow_o[index:index + 1, 0:n] = c_new
        q = jnp.sum(r_new, axis=1, keepdims=True) / m_all
        columns = to_columns(r_new)
        rc_o[...] = columns
        a = lax.rsqrt(columns / q)
        b_row = lax.rsqrt(c_new)
        acc = jnp.zeros((m, 128), F32)
        for lo in range(0, n, 128):
            u = g[:, lo:lo + 128] * (a * b_row[:, lo:lo + 128])
            acc = acc + u * u
        qs.append(q)
        ss.append(jnp.sum(jnp.sum(acc, axis=0, keepdims=True), axis=1, keepdims=True))

    lane = lax.broadcasted_iota(jnp.int32, (1, 128), 1)

    def lanes(values, fill):
        out = jnp.full((1, 128), fill, F32)
        for index, value in enumerate(values):
            out = jnp.where(lane == index, value, out)
        return out

    s2_send[...] = jnp.zeros_like(s2_send)
    s2_send[0:1, :] = lanes(qs, 1.0)
    s2_send[1:2, :] = lanes(ss, 0.0)
    s2_send[2:3, :] = lanes(w_sq, 0.0)
    s2 = []
    for k, (a, b) in enumerate(peers):
        copy = remote(s2_send, s2_recv.at[k], s2_ssem.at[k], s2_rsem.at[k], peer(a, b))
        copy.start()
        s2.append(copy)

    @pl.loop(0, steps)
    def _(i):
        rows_i = pl.ds(pl.multiple_of(i * CHUNK, CHUNK), CHUNK)
        p_copy(i).wait_recv()
        half_v[rows_i, :] = (p_own[rows_i, :] + p_recv[rows_i, :]).astype(BF16)

    store(half_v, half_o)

    for copy in s2:
        copy.wait_recv()
    table = [s2_send] + [s2_recv.at[k] for k in range(7)]

    def tree(values):
        while len(values) > 1:
            values = [values[k] + values[k + 1] for k in range(0, len(values), 2)]
        return values[0]

    r_mean = tree([t[0:1, :] for t in table[:4]])
    u_sq = []
    for t in table:
        ratio = jnp.sqrt(r_mean) / jnp.sqrt(t[0:1, :])
        u_sq.append((t[1:2, :] * ratio) * ratio)
    size = F32(shapes[0][0] * shapes[0][1] * 8)
    rms_u = jnp.sqrt(tree(u_sq) / size)
    step_size = hp[1] * jnp.maximum(EPS_TWO, jnp.sqrt(tree([t[2:3, :] for t in table]) / size))
    scal_o[...] = jnp.zeros_like(scal_o)
    scal_o[0:1, :] = r_mean
    scal_o[1:2, :] = 1.0 / jnp.maximum(1.0, rms_u / hp[2])
    scal_o[2:3, :] = step_size

    for copy in shares:
        copy.wait_recv()
    f3.wait_recv()
    for copy in [f1, f3, s1_row] + s1_col + shares + s2:
        copy.wait_send()

    @pl.loop(0, steps)
    def _(i):
        p_copy(i).wait_send()

    for copy in outs:
        copy.wait()


def update_kernel(
    gg, gu, gd, wg, wu, wd, rcg, rcu, rcd, rrow, crow, scal, wd_all, dyd_all,
    wg_o, wu_o, wd_o, dx_o, rg_o, cg_o, ru_o, cu_o, rd_o, cd_o,
):
    dx = dot(wd_all[0], dyd_all[0], NT) + dot(wd_all[1], dyd_all[1], NT)
    dx_o[...] = dx.astype(BF16)
    for index, (g, w, rc, out) in enumerate(((gg, wg, rcg, wg_o), (gu, wu, rcu, wu_o), (gd, wd, rcd, wd_o))):
        n = g.shape[1]
        r_mean = scal[0:1, index:index + 1]
        inv = scal[1:2, index:index + 1]
        step = scal[2:3, index:index + 1]
        a = lax.rsqrt(rc[...] / r_mean)
        b_row = lax.rsqrt(crow[index:index + 1, 0:n])
        for lo in range(0, n, 128):
            u = g[:, lo:lo + 128] * (a * b_row[:, lo:lo + 128])
            out[:, lo:lo + 128] = w[:, lo:lo + 128] - step * (u * inv)

    @pl.when(pl.program_id(0) == 0)
    def _():
        for index, (r_out, c_out) in enumerate(((rg_o, cg_o), (ru_o, cu_o), (rd_o, cd_o))):
            r_out[...] = rrow[index:index + 1, 0:r_out.shape[0]].reshape(r_out.shape)
            c_out[...] = crow[index:index + 1, 0:c_out.shape[0]].reshape(c_out.shape)


def solution(mesh):
    weight_spec = P('row', 'col')
    act_spec = P(None, 'row')
    grad_spec = P(None, 'col')
    in_specs = (weight_spec,) * 3 + (act_spec, act_spec) + (grad_spec,) * 3 + (P('row'), P('col')) * 3 + (P(),)
    out_specs = (weight_spec,) * 3 + (P('row'), P('col')) * 3 + (act_spec, act_spec)

    def body(w_gate, w_up, w_down, x_norm, x_act, dy_gate, dy_up, dy_down, r_gate, c_gate, r_up, c_up, r_down, c_down, hyper_params):
        m1, n1 = w_gate.shape
        m2, n2 = w_down.shape
        tokens = x_norm.shape[0]
        half = tokens // 2
        steps = half // CHUNK
        any_spec = pl.BlockSpec(memory_space=pl.ANY)
        vmem_spec = pl.BlockSpec(memory_space=pltpu.VMEM)
        sds = jax.ShapeDtypeStruct
        vm = pltpu.VMEM
        dma = pltpu.SemaphoreType.DMA
        outs = pl.pallas_call(
            functools.partial(exchange_kernel, m1),
            name="exchange",
            out_shape=[
                sds((m1, n1), F32), sds((m1, n1), F32), sds((m2, n2), F32),
                sds((2, m2, n2), BF16), sds((2, tokens, n2), BF16), sds((half, m1), BF16),
                sds((m1, 128), F32), sds((m1, 128), F32), sds((m2, 128), F32),
                sds((8, 768), F32), sds((8, n1), F32), sds((8, 128), F32),
            ],
            in_specs=[any_spec] * 8 + [vmem_spec] * 6 + [pl.BlockSpec(memory_space=pltpu.SMEM)],
            out_specs=[any_spec] * 6 + [vmem_spec] * 6,
            scratch_shapes=[
                vm((m1, n1), F32), vm((m1, n1), F32), vm((m2, n2), F32),
                vm((m1, n1), BF16), vm((m1, n1), BF16), vm((m2, n2), BF16),
                vm((tokens, n1), BF16), vm((tokens, n1), BF16), vm((tokens, n2), BF16),
                vm((tokens, m1), BF16), vm((m1, tokens), BF16), vm((m2, tokens), BF16),
                vm((m1, n1), F32), vm((m1, n1), F32), vm((m2, n2), F32),
                vm((half, m1), F32), vm((half, m1), F32), vm((half, m1), F32), vm((half, m1), BF16),
                vm((8, 768), F32), vm((8, 768), F32), vm((8, n1), F32), vm((3, 8, n1), F32),
                vm((8, 128), F32), vm((7, 8, 128), F32),
                dma((10,)), dma((6,)), dma((5,)), dma((5,)), dma((steps,)), dma((steps,)),
                dma((4,)), dma((4,)), dma((7,)), dma((7,)),
            ],
            compiler_params=pltpu.CompilerParams(
                collective_id=0, has_side_effects=True, vmem_limit_bytes=60 * 1024 * 1024
            ),
            cost_estimate=pl.CostEstimate(flops=30_000_000_000, bytes_accessed=40_000_000, transcendentals=0),
        )(w_gate, w_up, w_down, x_norm, x_act.T, dy_gate, dy_up, dy_down, r_gate, c_gate, r_up, c_up, r_down, c_down, hyper_params)
        gg, gu, gd, wd_all, dyd_all, own, rcg, rcu, rcd, rrow, crow, scal = outs

        other = lax.ppermute(own, 'col', [(0, 1), (1, 0)])

        grid = 8
        b1, b2, bt = m1 // grid, m2 // grid, tokens // grid

        def rows(*block):
            return pl.BlockSpec(block, lambda i: (i,) + (0,) * (len(block) - 1))

        def whole(*block):
            return pl.BlockSpec(block, lambda i: (0,) * len(block))

        wide, tall = rows(b1, n1), rows(b2, n2)
        new_gate, new_up, new_down, dx_act, rg, cg, ru, cu, rd, cd = pl.pallas_call(
            update_kernel,
            name="update",
            grid=(grid,),
            out_shape=[
                sds((m1, n1), F32), sds((m1, n1), F32), sds((m2, n2), F32), sds((m2, tokens), BF16),
                sds((m1,), F32), sds((n1,), F32), sds((m1,), F32), sds((n1,), F32), sds((m2,), F32), sds((n2,), F32),
            ],
            in_specs=[wide, wide, tall, wide, wide, tall, rows(b1, 128), rows(b1, 128), rows(b2, 128),
                      whole(8, 768), whole(8, n1), whole(8, 128), whole(2, m2, n2),
                      pl.BlockSpec((2, bt, n2), lambda i: (0, i, 0))],
            out_specs=[wide, wide, tall, pl.BlockSpec((m2, bt), lambda i: (0, i)),
                       whole(m1), whole(n1), whole(m1), whole(n1), whole(m2), whole(n2)],
            compiler_params=pltpu.CompilerParams(vmem_limit_bytes=48 * 1024 * 1024),
            cost_estimate=pl.CostEstimate(flops=4 * tokens * m2 * n2, bytes_accessed=22_000_000, transcendentals=0),
        )(gg, gu, gd, w_gate, w_up, w_down, rcg, rcu, rcd, rrow, crow, scal, wd_all, dyd_all)

        first = lax.axis_index('col') == 0
        dx_norm = jnp.where(first, jnp.concatenate([own, other]), jnp.concatenate([other, own]))
        return (new_gate, new_up, new_down, rg, cg, ru, cu, rd, cd, dx_norm, dx_act.T)

    return jax.shard_map(body, mesh=mesh, in_specs=in_specs, out_specs=out_specs, check_vma=False)
```

```python
import jax
import jax.numpy as jnp
from jax import lax
from jax.experimental import pallas as pl
from jax.experimental.pallas import tpu as pltpu
from jax.sharding import PartitionSpec as P

EPS_ONE = 1e-30
EPS_TWO = 1e-3
MESH = pl.DeviceIdType.MESH
F32 = jnp.float32
BF16 = jnp.bfloat16
NT = (((1,), (1,)), ((), ()))
CHUNK = 256


def dot(a, b, dims=(((1,), (0,)), ((), ()))):
    return lax.dot_general(a, b, dims, preferred_element_type=F32)


def spans(total, step):
    return [(lo, min(step, total - lo)) for lo in range(0, total, step)]


def to_row(column):
    return jnp.transpose(jnp.broadcast_to(column, (column.shape[0], 128)))[0:1, :]


def to_columns(row):
    return jnp.transpose(jnp.broadcast_to(row, (128, row.shape[1])))


def exchange_kernel(
    wg, wu, wd, xn, xat, dyg, dyu, dyd, rg, cg, ru, cu, rd, cd, hp,
    gg_o, gu_o, gd_o, wd_o, dyd_o, half_o, rcg_o, rcu_o, rcd_o, rrow_o, crow_o, scal_o,
    wg_v, wu_v, wd_v, wgb, wub, wdb, dyg_v, dyu_v, dyd_v, xn_v, xnt, xat_v, g_g, g_u, g_d,
    p_send, p_recv, p_own, half_v, rs_send, rs_recv, cs_send, cs_recv, s2_send, s2_recv,
    rg_v, cg_v, ru_v, cu_v, rd_v, cd_v, rcg_v, rcu_v, rcd_v, rrow_v, crow_v, scal_v,
    in_sem, out_sem, bulk_send, bulk_recv, p_ssem, p_rsem, st_send, st_recv, s2_ssem, s2_rsem,
):
    c = lax.axis_index("col")
    r = lax.axis_index("row")
    rows = {0: r, 1: r + 1 - 2 * (r % 2), 2: (r + 2) % 4, 3: 3 - r}
    cols = {0: c, 1: 1 - c}
    peers = [(a, b) for a in (0, 1) for b in (0, 1, 2, 3) if (a, b) != (0, 0)]

    def peer(a, b):
        return (cols[a], rows[b])

    def remote(src, dst, ssem, rsem, who):
        return pltpu.make_async_remote_copy(
            src_ref=src, dst_ref=dst, send_sem=ssem, recv_sem=rsem, device_id=who, device_id_type=MESH
        )

    tokens = dyg.shape[0]
    half = tokens // 2
    quarter = tokens // 4
    steps = half // CHUNK
    mine, theirs = pl.multiple_of(c * half, half), pl.multiple_of((1 - c) * half, half)

    loads = []

    def load(src, dst):
        copy = pltpu.make_async_copy(src, dst, in_sem.at[len(loads)])
        copy.start()
        loads.append(copy)
        return copy

    l_wg = load(wg, wg_v)
    l_wu = load(wu, wu_v)
    l_dg1 = load(dyg.at[pl.ds(theirs, half)], dyg_v.at[pl.ds(theirs, half)])
    l_du1 = load(dyu.at[pl.ds(theirs, half)], dyu_v.at[pl.ds(theirs, half)])
    l_xn = load(xn, xn_v)
    l_dg2 = load(dyg.at[pl.ds(mine, half)], dyg_v.at[pl.ds(mine, half)])
    l_du2 = load(dyu.at[pl.ds(mine, half)], dyu_v.at[pl.ds(mine, half)])
    l_xat = load(xat, xat_v)
    l_dyd = load(dyd, dyd_v)
    l_wd = load(wd, wd_v)
    l_small = [load(src, dst) for src, dst in ((rg, rg_v), (cg, cg_v), (ru, ru_v), (cu, cu_v), (rd, rd_v), (cd, cd_v))]

    barrier = pltpu.get_barrier_semaphore()
    for a, b in peers:
        pl.semaphore_signal(barrier, inc=1, device_id=peer(a, b), device_id_type=MESH)
    pl.semaphore_wait(barrier, 7)

    my_rows = pl.ds(pl.multiple_of(r * quarter, quarter), quarter)
    f1 = remote(dyd.at[my_rows], dyd_o.at[c, my_rows], bulk_send.at[0], bulk_recv.at[0], peer(1, 0))
    f1.start()

    outs = []

    def store(src, dst):
        copy = pltpu.make_async_copy(src, dst, out_sem.at[len(outs)])
        copy.start()
        outs.append(copy)

    l_wg.wait()
    wgb[...] = wg_v[...].astype(BF16)
    l_wu.wait()
    wub[...] = wu_v[...].astype(BF16)
    l_dg1.wait()
    l_du1.wait()

    def p_copy(i):
        rows_i = pl.ds(pl.multiple_of(i * CHUNK, CHUNK), CHUNK)
        return remote(p_send.at[rows_i], p_recv.at[rows_i], p_ssem.at[i], p_rsem.at[i], peer(1, 0))

    def partial(base, i):
        rows_i = pl.ds(pl.multiple_of(base + i * CHUNK, CHUNK), CHUNK)
        return dot(dyg_v[rows_i, :], wgb[...], NT) + dot(dyu_v[rows_i, :], wub[...], NT)

    def send_partial(i):
        p_send[pl.ds(pl.multiple_of(i * CHUNK, CHUNK), CHUNK), :] = partial(theirs, i)
        p_copy(i).start()

    pl.loop(0, steps // 2)(send_partial)

    rs_send[...] = jnp.zeros_like(rs_send)
    cs_send[...] = jnp.zeros_like(cs_send)
    l_xn.wait()
    for lo, width in spans(tokens, 256):
        xnt[:, lo:lo + width] = jnp.transpose(xn_v[lo:lo + width, :])
    l_dg2.wait()
    l_du2.wait()

    def gradient(index, lhs, rhs, out):
        m, n = out.shape
        acc = jnp.zeros((m, 128), F32)
        for lo, width in spans(n, 256):
            g = dot(lhs[...], rhs[:, lo:lo + width])
            out[:, lo:lo + width] = g
            sq = g * g + EPS_ONE
            cs_send[index:index + 1, lo:lo + width] = jnp.sum(sq, axis=0, keepdims=True)
            for part in range(0, width, 128):
                acc = acc + sq[:, part:part + 128]
        rs_send[index:index + 1, 0:m] = to_row(jnp.sum(acc, axis=1, keepdims=True))

    gradient(0, xnt, dyg_v, g_g)
    gradient(1, xnt, dyu_v, g_u)
    l_xat.wait()
    l_dyd.wait()
    gradient(2, xat_v, dyd_v, g_d)

    s1_row = remote(rs_send, rs_recv, st_send.at[0], st_recv.at[0], peer(1, 0))
    s1_row.start()
    s1_col = []
    for b in (1, 2, 3):
        copy = remote(cs_send, cs_recv.at[b - 1], st_send.at[b], st_recv.at[b], peer(0, b))
        copy.start()
        s1_col.append(copy)

    store(g_g, gg_o)
    store(g_u, gu_o)
    store(g_d, gd_o)
    store(dyd_v, dyd_o.at[c])

    pl.loop(steps // 2, steps)(send_partial)

    l_wd.wait()
    wdb[...] = wd_v[...].astype(BF16)
    store(wdb, wd_o)

    w_sq = [jnp.sum(jnp.sum(w[...] * w[...], axis=0, keepdims=True), axis=1, keepdims=True) for w in (wg_v, wu_v, wd_v)]

    f1.wait_recv()
    shares = []
    for b in (1, 2, 3):
        copy = remote(dyd_o.at[1 - c, my_rows], dyd_o.at[1 - c, my_rows], bulk_send.at[b], bulk_recv.at[b], peer(0, b))
        copy.start()
        shares.append(copy)

    @pl.loop(0, steps)
    def _(i):
        p_own[pl.ds(pl.multiple_of(i * CHUNK, CHUNK), CHUNK), :] = partial(mine, i)

    s1_row.wait_recv()
    for copy in s1_col:
        copy.wait_recv()
    beta = hp[0]
    for copy in l_small:
        copy.wait()
    shapes = [g.shape for g in (g_g, g_u, g_d)]
    qs, ss = [], []
    rrow_v[...] = jnp.zeros_like(rrow_v)
    crow_v[...] = jnp.ones_like(crow_v)
    for index, (g, r_ref, c_ref, rc_v) in enumerate(((g_g, rg_v, cg_v, rcg_v), (g_u, ru_v, cu_v, rcu_v), (g_d, rd_v, cd_v, rcd_v))):
        m, n = shapes[index]
        m_all, n_all = m * 4, n * 2
        row_sum = rs_send[index:index + 1, 0:m] + rs_recv[index:index + 1, 0:m]
        col_sum = (cs_send[index:index + 1, 0:n] + cs_recv[0, index:index + 1, 0:n]) + (
            cs_recv[1, index:index + 1, 0:n] + cs_recv[2, index:index + 1, 0:n])
        r_new = beta * r_ref[...].reshape(1, m) + (1.0 - beta) * (row_sum / n_all)
        c_new = beta * c_ref[...].reshape(1, n) + (1.0 - beta) * (col_sum / m_all)
        rrow_v[index:index + 1, 0:m] = r_new
        crow_v[index:index + 1, 0:n] = c_new
        q = jnp.sum(r_new, axis=1, keepdims=True) / m_all
        columns = to_columns(r_new)
        rc_v[...] = columns
        a = lax.rsqrt(columns / q)
        b_row = lax.rsqrt(c_new)
        acc = jnp.zeros((m, 128), F32)
        for lo in range(0, n, 128):
            u = g[:, lo:lo + 128] * (a * b_row[:, lo:lo + 128])
            acc = acc + u * u
        qs.append(q)
        ss.append(jnp.sum(jnp.sum(acc, axis=0, keepdims=True), axis=1, keepdims=True))

    lane = lax.broadcasted_iota(jnp.int32, (1, 128), 1)

    def lanes(values, fill):
        out = jnp.full((1, 128), fill, F32)
        for index, value in enumerate(values):
            out = jnp.where(lane == index, value, out)
        return out

    s2_send[...] = jnp.zeros_like(s2_send)
    s2_send[0:1, :] = lanes(qs, 1.0)
    s2_send[1:2, :] = lanes(ss, 0.0)
    s2_send[2:3, :] = lanes(w_sq, 0.0)
    s2 = []
    for k, (a, b) in enumerate(peers):
        copy = remote(s2_send, s2_recv.at[k], s2_ssem.at[k], s2_rsem.at[k], peer(a, b))
        copy.start()
        s2.append(copy)

    for src, dst in ((rcg_v, rcg_o), (rcu_v, rcu_o), (rcd_v, rcd_o), (rrow_v, rrow_o), (crow_v, crow_o)):
        store(src, dst)

    @pl.loop(0, steps)
    def _(i):
        rows_i = pl.ds(pl.multiple_of(i * CHUNK, CHUNK), CHUNK)
        p_copy(i).wait_recv()
        half_v[rows_i, :] = (p_own[rows_i, :] + p_recv[rows_i, :]).astype(BF16)

    store(half_v, half_o)

    for copy in s2:
        copy.wait_recv()
    table = [s2_send] + [s2_recv.at[k] for k in range(7)]

    def tree(values):
        while len(values) > 1:
            values = [values[k] + values[k + 1] for k in range(0, len(values), 2)]
        return values[0]

    r_mean = tree([t[0:1, :] for t in table[:4]])
    u_sq = []
    for t in table:
        ratio = jnp.sqrt(r_mean) / jnp.sqrt(t[0:1, :])
        u_sq.append((t[1:2, :] * ratio) * ratio)
    size = F32(shapes[0][0] * shapes[0][1] * 8)
    rms_u = jnp.sqrt(tree(u_sq) / size)
    step_size = hp[1] * jnp.maximum(EPS_TWO, jnp.sqrt(tree([t[2:3, :] for t in table]) / size))
    scal_v[...] = jnp.zeros_like(scal_v)
    scal_v[0:1, :] = r_mean
    scal_v[1:2, :] = 1.0 / jnp.maximum(1.0, rms_u / hp[2])
    scal_v[2:3, :] = step_size
    store(scal_v, scal_o)

    for copy in shares:
        copy.wait_recv()
    for copy in [f1, s1_row] + s1_col + shares + s2:
        copy.wait_send()

    @pl.loop(0, steps)
    def _(i):
        p_copy(i).wait_send()

    for copy in outs:
        copy.wait()


def update_kernel(
    gg, gu, gd, wg, wu, wd, rcg, rcu, rcd, rrow, crow, scal, own,
    wg_o, wu_o, wd_o, dxn_o, rg_o, cg_o, ru_o, cu_o, rd_o, cd_o, sem,
):
    half = own.shape[0]
    rows = pl.ds(pl.multiple_of(lax.axis_index("col") * half, half), half)
    copy = pltpu.make_async_copy(own, dxn_o.at[rows], sem)

    @pl.when(pl.program_id(0) == 0)
    def _():
        copy.start()
        for index, (r_out, c_out) in enumerate(((rg_o, cg_o), (ru_o, cu_o), (rd_o, cd_o))):
            r_out[...] = rrow[index:index + 1, 0:r_out.shape[0]].reshape(r_out.shape)
            c_out[...] = crow[index:index + 1, 0:c_out.shape[0]].reshape(c_out.shape)

    for index, (g, w, rc, out) in enumerate(((gg, wg, rcg, wg_o), (gu, wu, rcu, wu_o), (gd, wd, rcd, wd_o))):
        n = g.shape[1]
        r_mean = scal[0:1, index:index + 1]
        inv = scal[1:2, index:index + 1]
        step = scal[2:3, index:index + 1]
        a = lax.rsqrt(rc[...] / r_mean)
        b_row = lax.rsqrt(crow[index:index + 1, 0:n])
        for lo in range(0, n, 128):
            u = g[:, lo:lo + 128] * (a * b_row[:, lo:lo + 128])
            out[:, lo:lo + 128] = w[:, lo:lo + 128] - step * (u * inv)

    @pl.when(pl.program_id(0) == pl.num_programs(0) - 1)
    def _():
        copy.wait()


def input_grad_kernel(own, other, dyd_all, dx_o):
    def emit(first, second):
        dx = dot(first[...], dyd_all[0], NT) + dot(second[...], dyd_all[1], NT)
        dx_o[...] = dx.astype(BF16)

    c = lax.axis_index("col")
    pl.when(c == 0)(lambda: emit(own, other))
    pl.when(c == 1)(lambda: emit(other, own))


def solution(mesh):
    weight_spec = P('row', 'col')
    act_spec = P(None, 'row')
    grad_spec = P(None, 'col')
    in_specs = (weight_spec,) * 3 + (act_spec, act_spec) + (grad_spec,) * 3 + (P('row'), P('col')) * 3 + (P(),)
    out_specs = (weight_spec,) * 3 + (P('row'), P('col')) * 3 + (act_spec, act_spec)

    def body(w_gate, w_up, w_down, x_norm, x_act, dy_gate, dy_up, dy_down, r_gate, c_gate, r_up, c_up, r_down, c_down, hyper_params):
        m1, n1 = w_gate.shape
        m2, n2 = w_down.shape
        tokens = x_norm.shape[0]
        half = tokens // 2
        steps = half // CHUNK
        any_spec = pl.BlockSpec(memory_space=pl.ANY)
        sds = jax.ShapeDtypeStruct
        vm = pltpu.VMEM
        dma = pltpu.SemaphoreType.DMA
        outs = pl.pallas_call(
            exchange_kernel,
            name="exchange",
            out_shape=[
                sds((m1, n1), F32), sds((m1, n1), F32), sds((m2, n2), F32),
                sds((m2, n2), BF16), sds((2, tokens, n2), BF16), sds((half, m1), BF16),
                sds((m1, 128), F32), sds((m1, 128), F32), sds((m2, 128), F32),
                sds((8, 768), F32), sds((8, n1), F32), sds((8, 128), F32),
            ],
            in_specs=[any_spec] * 14 + [pl.BlockSpec(memory_space=pltpu.SMEM)],
            out_specs=[any_spec] * 12,
            scratch_shapes=[
                vm((m1, n1), F32), vm((m1, n1), F32), vm((m2, n2), F32),
                vm((m1, n1), BF16), vm((m1, n1), BF16), vm((m2, n2), BF16),
                vm((tokens, n1), BF16), vm((tokens, n1), BF16), vm((tokens, n2), BF16),
                vm((tokens, m1), BF16), vm((m1, tokens), BF16), vm((m2, tokens), BF16),
                vm((m1, n1), F32), vm((m1, n1), F32), vm((m2, n2), F32),
                vm((half, m1), F32), vm((half, m1), F32), vm((half, m1), F32), vm((half, m1), BF16),
                vm((8, 768), F32), vm((8, 768), F32), vm((8, n1), F32), vm((3, 8, n1), F32),
                vm((8, 128), F32), vm((7, 8, 128), F32),
                vm((m1,), F32), vm((n1,), F32), vm((m1,), F32), vm((n1,), F32), vm((m2,), F32), vm((n2,), F32),
                vm((m1, 128), F32), vm((m1, 128), F32), vm((m2, 128), F32),
                vm((8, 768), F32), vm((8, n1), F32), vm((8, 128), F32),
                dma((16,)), dma((12,)), dma((4,)), dma((4,)), dma((steps,)), dma((steps,)),
                dma((4,)), dma((4,)), dma((7,)), dma((7,)),
            ],
            compiler_params=pltpu.CompilerParams(
                collective_id=0, has_side_effects=True, vmem_limit_bytes=60 * 1024 * 1024
            ),
            cost_estimate=pl.CostEstimate(flops=30_000_000_000, bytes_accessed=40_000_000, transcendentals=0),
        )(w_gate, w_up, w_down, x_norm, x_act.T, dy_gate, dy_up, dy_down, r_gate, c_gate, r_up, c_up, r_down, c_down, hyper_params)
        gg, gu, gd, wd_own, dyd_all, own, rcg, rcu, rcd, rrow, crow, scal = outs
        pairs = [(0, 1), (1, 0)]
        wd_other = lax.ppermute(wd_own, 'col', pairs)
        other = lax.ppermute(own, 'col', pairs)

        def rows(*block):
            return pl.BlockSpec(block, lambda i: (i,) + (0,) * (len(block) - 1))

        def whole(*block):
            return pl.BlockSpec(block, lambda i: (0,) * len(block))

        grid = 4
        b1, b2, bt = m1 // grid, m2 // grid, tokens // grid
        wide, tall = rows(b1, n1), rows(b2, n2)
        new_gate, new_up, new_down, dx_norm, rg, cg, ru, cu, rd, cd = pl.pallas_call(
            update_kernel,
            name="update",
            grid=(grid,),
            out_shape=[
                sds((m1, n1), F32), sds((m1, n1), F32), sds((m2, n2), F32), sds((tokens, m1), BF16),
                sds((m1,), F32), sds((n1,), F32), sds((m1,), F32), sds((n1,), F32), sds((m2,), F32), sds((n2,), F32),
            ],
            in_specs=[wide, wide, tall, wide, wide, tall, rows(b1, 128), rows(b1, 128), rows(b2, 128),
                      whole(8, 768), whole(8, n1), whole(8, 128), whole(half, m1)],
            out_specs=[wide, wide, tall, any_spec,
                       whole(m1), whole(n1), whole(m1), whole(n1), whole(m2), whole(n2)],
            scratch_shapes=[dma],
            compiler_params=pltpu.CompilerParams(vmem_limit_bytes=67043328),
            cost_estimate=pl.CostEstimate(flops=3_000_000_000, bytes_accessed=14_000_000, transcendentals=0),
        )(gg, gu, gd, w_gate, w_up, w_down, rcg, rcu, rcd, rrow, crow, scal, own)

        dx_act = pl.pallas_call(
            input_grad_kernel,
            name="input_grad",
            grid=(grid,),
            out_shape=sds((m2, tokens), BF16),
            in_specs=[whole(m2, n2), whole(m2, n2), pl.BlockSpec((2, bt, n2), lambda i: (0, i, 0))],
            out_specs=pl.BlockSpec((m2, bt), lambda i: (0, i)),
            compiler_params=pltpu.CompilerParams(vmem_limit_bytes=67043328),
            cost_estimate=pl.CostEstimate(flops=4 * tokens * m2 * n2, bytes_accessed=9_000_000, transcendentals=0),
        )(wd_own, wd_other, dyd_all)

        start = (1 - lax.axis_index('col')) * half
        dx_norm = lax.dynamic_update_slice(dx_norm, other, (start, 0))
        return (new_gate, new_up, new_down, rg, cg, ru, cu, rd, cd, dx_norm, dx_act.T)

    return jax.shard_map(body, mesh=mesh, in_specs=in_specs, out_specs=out_specs, check_vma=False)
```

```python
import jax
import jax.numpy as jnp
from jax import lax
from jax.experimental import pallas as pl
from jax.experimental.pallas import tpu as pltpu
from jax.sharding import PartitionSpec as P

EPS_ONE = 1e-30
EPS_TWO = 1e-3
MESH = pl.DeviceIdType.MESH
F32 = jnp.float32
BF16 = jnp.bfloat16
NT = (((1,), (1,)), ((), ()))
CHUNK = 256


def dot(a, b, dims=(((1,), (0,)), ((), ()))):
    return lax.dot_general(a, b, dims, preferred_element_type=F32)


def spans(total, step):
    return [(lo, min(step, total - lo)) for lo in range(0, total, step)]


def to_row(column):
    return jnp.transpose(jnp.broadcast_to(column, (column.shape[0], 128)))[0:1, :]


def to_columns(row):
    return jnp.transpose(jnp.broadcast_to(row, (128, row.shape[1])))


def exchange_kernel(
    wg, wu, wd, xn, xat, dyg, dyu, dyd, rg, cg, ru, cu, rd, cd, hp,
    gg_o, gu_o, gd_o, wd_o, dyd_o, half_o, rcg_o, rcu_o, rcd_o, rrow_o, crow_o, scal_o,
    wg_v, wu_v, wd_v, wgb, wub, wdb, dyg_v, dyu_v, dyd_v, xn_v, xnt, xat_v, g_g, g_u, g_d,
    p_send, p_recv, p_own, half_v, rs_send, rs_recv, cs_send, cs_recv, s2_send, s2_recv,
    rg_v, cg_v, ru_v, cu_v, rd_v, cd_v, rcg_v, rcu_v, rcd_v, rrow_v, crow_v, scal_v,
    in_sem, out_sem, bulk_send, bulk_recv, p_ssem, p_rsem, st_send, st_recv, s2_ssem, s2_rsem,
):
    c = lax.axis_index("col")
    r = lax.axis_index("row")
    rows = {0: r, 1: r + 1 - 2 * (r % 2), 2: (r + 2) % 4, 3: 3 - r}
    cols = {0: c, 1: 1 - c}
    peers = [(a, b) for a in (0, 1) for b in (0, 1, 2, 3) if (a, b) != (0, 0)]

    def peer(a, b):
        return (cols[a], rows[b])

    def remote(src, dst, ssem, rsem, who):
        return pltpu.make_async_remote_copy(
            src_ref=src, dst_ref=dst, send_sem=ssem, recv_sem=rsem, device_id=who, device_id_type=MESH
        )

    tokens = dyg.shape[0]
    half = tokens // 2
    quarter = tokens // 4
    steps = half // CHUNK
    mine, theirs = pl.multiple_of(c * half, half), pl.multiple_of((1 - c) * half, half)

    loads = []

    def load(src, dst):
        copy = pltpu.make_async_copy(src, dst, in_sem.at[len(loads)])
        copy.start()
        loads.append(copy)
        return copy

    l_wg = load(wg, wg_v)
    l_wu = load(wu, wu_v)
    l_dg1 = load(dyg.at[pl.ds(theirs, half)], dyg_v.at[pl.ds(theirs, half)])
    l_du1 = load(dyu.at[pl.ds(theirs, half)], dyu_v.at[pl.ds(theirs, half)])
    l_xn = load(xn, xn_v)
    l_dg2 = load(dyg.at[pl.ds(mine, half)], dyg_v.at[pl.ds(mine, half)])
    l_du2 = load(dyu.at[pl.ds(mine, half)], dyu_v.at[pl.ds(mine, half)])
    l_xat = load(xat, xat_v)
    l_dyd = load(dyd, dyd_v)
    l_wd = load(wd, wd_v)
    l_small = [load(src, dst) for src, dst in ((rg, rg_v), (cg, cg_v), (ru, ru_v), (cu, cu_v), (rd, rd_v), (cd, cd_v))]

    barrier = pltpu.get_barrier_semaphore()
    for a, b in peers:
        pl.semaphore_signal(barrier, inc=1, device_id=peer(a, b), device_id_type=MESH)
    pl.semaphore_wait(barrier, 7)

    my_rows = pl.ds(pl.multiple_of(r * quarter, quarter), quarter)
    f1 = remote(dyd.at[my_rows], dyd_o.at[c, my_rows], bulk_send.at[0], bulk_recv.at[0], peer(1, 0))
    f1.start()

    outs = []

    def store(src, dst):
        copy = pltpu.make_async_copy(src, dst, out_sem.at[len(outs)])
        copy.start()
        outs.append(copy)

    l_wg.wait()
    wgb[...] = wg_v[...].astype(BF16)
    l_wu.wait()
    wub[...] = wu_v[...].astype(BF16)
    l_dg1.wait()
    l_du1.wait()

    def p_copy(i):
        rows_i = pl.ds(pl.multiple_of(i * CHUNK, CHUNK), CHUNK)
        return remote(p_send.at[rows_i], p_recv.at[rows_i], p_ssem.at[i], p_rsem.at[i], peer(1, 0))

    def partial(base, i):
        rows_i = pl.ds(pl.multiple_of(base + i * CHUNK, CHUNK), CHUNK)
        return dot(dyg_v[rows_i, :], wgb[...], NT) + dot(dyu_v[rows_i, :], wub[...], NT)

    def send_partial(i):
        p_send[pl.ds(pl.multiple_of(i * CHUNK, CHUNK), CHUNK), :] = partial(theirs, i)
        p_copy(i).start()

    pl.loop(0, steps // 2)(send_partial)

    rs_send[...] = jnp.zeros_like(rs_send)
    cs_send[...] = jnp.zeros_like(cs_send)
    l_xn.wait()
    for lo, width in spans(tokens, 256):
        xnt[:, lo:lo + width] = jnp.transpose(xn_v[lo:lo + width, :])
    l_dg2.wait()
    l_du2.wait()

    def gradient(index, lhs, rhs, out):
        m, n = out.shape
        acc = jnp.zeros((m, 128), F32)
        for lo, width in spans(n, 256):
            g = dot(lhs[...], rhs[:, lo:lo + width])
            out[:, lo:lo + width] = g
            sq = g * g + EPS_ONE
            cs_send[index:index + 1, lo:lo + width] = jnp.sum(sq, axis=0, keepdims=True)
            for part in range(0, width, 128):
                acc = acc + sq[:, part:part + 128]
        rs_send[index:index + 1, 0:m] = to_row(jnp.sum(acc, axis=1, keepdims=True))

    gradient(0, xnt, dyg_v, g_g)
    gradient(1, xnt, dyu_v, g_u)
    l_xat.wait()
    l_dyd.wait()
    gradient(2, xat_v, dyd_v, g_d)

    s1_row = remote(rs_send, rs_recv, st_send.at[0], st_recv.at[0], peer(1, 0))
    s1_row.start()
    s1_col = []
    for b in (1, 2, 3):
        copy = remote(cs_send, cs_recv.at[b - 1], st_send.at[b], st_recv.at[b], peer(0, b))
        copy.start()
        s1_col.append(copy)

    store(g_g, gg_o)
    store(g_u, gu_o)
    store(g_d, gd_o)
    store(dyd_v, dyd_o.at[c])

    pl.loop(steps // 2, steps)(send_partial)

    l_wd.wait()
    wdb[...] = wd_v[...].astype(BF16)
    store(wdb, wd_o)

    w_sq = [jnp.sum(jnp.sum(w[...] * w[...], axis=0, keepdims=True), axis=1, keepdims=True) for w in (wg_v, wu_v, wd_v)]

    f1.wait_recv()
    shares = []
    for b in (1, 2):
        copy = remote(dyd_o.at[1 - c, my_rows], dyd_o.at[1 - c, my_rows], bulk_send.at[b], bulk_recv.at[b], peer(0, b))
        copy.start()
        shares.append(copy)

    @pl.loop(0, steps)
    def _(i):
        p_own[pl.ds(pl.multiple_of(i * CHUNK, CHUNK), CHUNK), :] = partial(mine, i)

    s1_row.wait_recv()
    for copy in s1_col:
        copy.wait_recv()
    beta = hp[0]
    for copy in l_small:
        copy.wait()
    shapes = [g.shape for g in (g_g, g_u, g_d)]
    qs, ss = [], []
    rrow_v[...] = jnp.zeros_like(rrow_v)
    crow_v[...] = jnp.ones_like(crow_v)
    for index, (g, r_ref, c_ref, rc_v) in enumerate(((g_g, rg_v, cg_v, rcg_v), (g_u, ru_v, cu_v, rcu_v), (g_d, rd_v, cd_v, rcd_v))):
        m, n = shapes[index]
        m_all, n_all = m * 4, n * 2
        row_sum = rs_send[index:index + 1, 0:m] + rs_recv[index:index + 1, 0:m]
        col_sum = (cs_send[index:index + 1, 0:n] + cs_recv[0, index:index + 1, 0:n]) + (
            cs_recv[1, index:index + 1, 0:n] + cs_recv[2, index:index + 1, 0:n])
        r_new = beta * r_ref[...].reshape(1, m) + (1.0 - beta) * (row_sum / n_all)
        c_new = beta * c_ref[...].reshape(1, n) + (1.0 - beta) * (col_sum / m_all)
        rrow_v[index:index + 1, 0:m] = r_new
        crow_v[index:index + 1, 0:n] = c_new
        q = jnp.sum(r_new, axis=1, keepdims=True) / m_all
        columns = to_columns(r_new)
        rc_v[...] = columns
        a = lax.rsqrt(columns / q)
        b_row = lax.rsqrt(c_new)
        acc = jnp.zeros((m, 128), F32)
        for lo in range(0, n, 128):
            u = g[:, lo:lo + 128] * (a * b_row[:, lo:lo + 128])
            acc = acc + u * u
        qs.append(q)
        ss.append(jnp.sum(jnp.sum(acc, axis=0, keepdims=True), axis=1, keepdims=True))

    lane = lax.broadcasted_iota(jnp.int32, (1, 128), 1)

    def lanes(values, fill):
        out = jnp.full((1, 128), fill, F32)
        for index, value in enumerate(values):
            out = jnp.where(lane == index, value, out)
        return out

    s2_send[...] = jnp.zeros_like(s2_send)
    s2_send[0:1, :] = lanes(qs, 1.0)
    s2_send[1:2, :] = lanes(ss, 0.0)
    s2_send[2:3, :] = lanes(w_sq, 0.0)
    s2 = []
    for k, (a, b) in enumerate(peers):
        copy = remote(s2_send, s2_recv.at[k], s2_ssem.at[k], s2_rsem.at[k], peer(a, b))
        copy.start()
        s2.append(copy)

    for src, dst in ((rcg_v, rcg_o), (rcu_v, rcu_o), (rcd_v, rcd_o), (rrow_v, rrow_o), (crow_v, crow_o)):
        store(src, dst)

    shares[1].wait_recv()
    at = pl.ds(pl.multiple_of(rows[2] * quarter, quarter), quarter)
    relay = remote(dyd_o.at[1 - c, at], dyd_o.at[1 - c, at], bulk_send.at[3], bulk_recv.at[3], peer(0, 1))
    relay.start()
    shares.append(relay)

    @pl.loop(0, steps)
    def _(i):
        rows_i = pl.ds(pl.multiple_of(i * CHUNK, CHUNK), CHUNK)
        p_copy(i).wait_recv()
        half_v[rows_i, :] = (p_own[rows_i, :] + p_recv[rows_i, :]).astype(BF16)

    store(half_v, half_o)

    for copy in s2:
        copy.wait_recv()
    table = [s2_send] + [s2_recv.at[k] for k in range(7)]

    def tree(values):
        while len(values) > 1:
            values = [values[k] + values[k + 1] for k in range(0, len(values), 2)]
        return values[0]

    r_mean = tree([t[0:1, :] for t in table[:4]])
    u_sq = []
    for t in table:
        ratio = jnp.sqrt(r_mean) / jnp.sqrt(t[0:1, :])
        u_sq.append((t[1:2, :] * ratio) * ratio)
    size = F32(shapes[0][0] * shapes[0][1] * 8)
    rms_u = jnp.sqrt(tree(u_sq) / size)
    step_size = hp[1] * jnp.maximum(EPS_TWO, jnp.sqrt(tree([t[2:3, :] for t in table]) / size))
    scal_v[...] = jnp.zeros_like(scal_v)
    scal_v[0:1, :] = r_mean
    scal_v[1:2, :] = 1.0 / jnp.maximum(1.0, rms_u / hp[2])
    scal_v[2:3, :] = step_size
    store(scal_v, scal_o)

    for copy in (shares[0], relay):
        copy.wait_recv()
    for copy in [f1, s1_row] + s1_col + shares + s2:
        copy.wait_send()

    @pl.loop(0, steps)
    def _(i):
        p_copy(i).wait_send()

    for copy in outs:
        copy.wait()


def update_kernel(
    gg, gu, gd, wg, wu, wd, rcg, rcu, rcd, rrow, crow, scal, own,
    wg_o, wu_o, wd_o, dxn_o, rg_o, cg_o, ru_o, cu_o, rd_o, cd_o, sem,
):
    half = own.shape[0]
    rows = pl.ds(pl.multiple_of(lax.axis_index("col") * half, half), half)
    copy = pltpu.make_async_copy(own, dxn_o.at[rows], sem)

    @pl.when(pl.program_id(0) == 0)
    def _():
        copy.start()
        for index, (r_out, c_out) in enumerate(((rg_o, cg_o), (ru_o, cu_o), (rd_o, cd_o))):
            r_out[...] = rrow[index:index + 1, 0:r_out.shape[0]].reshape(r_out.shape)
            c_out[...] = crow[index:index + 1, 0:c_out.shape[0]].reshape(c_out.shape)

    for index, (g, w, rc, out) in enumerate(((gg, wg, rcg, wg_o), (gu, wu, rcu, wu_o), (gd, wd, rcd, wd_o))):
        n = g.shape[1]
        r_mean = scal[0:1, index:index + 1]
        inv = scal[1:2, index:index + 1]
        step = scal[2:3, index:index + 1]
        a = lax.rsqrt(rc[...] / r_mean)
        b_row = lax.rsqrt(crow[index:index + 1, 0:n])
        for lo in range(0, n, 128):
            u = g[:, lo:lo + 128] * (a * b_row[:, lo:lo + 128])
            out[:, lo:lo + 128] = w[:, lo:lo + 128] - step * (u * inv)

    @pl.when(pl.program_id(0) == pl.num_programs(0) - 1)
    def _():
        copy.wait()


def input_grad_kernel(own, other, dyd_all, dx_o):
    def emit(first, second):
        dx = dot(first[...], dyd_all[0], NT) + dot(second[...], dyd_all[1], NT)
        dx_o[...] = dx.astype(BF16)

    c = lax.axis_index("col")
    pl.when(c == 0)(lambda: emit(own, other))
    pl.when(c == 1)(lambda: emit(other, own))


def solution(mesh):
    weight_spec = P('row', 'col')
    act_spec = P(None, 'row')
    grad_spec = P(None, 'col')
    in_specs = (weight_spec,) * 3 + (act_spec, act_spec) + (grad_spec,) * 3 + (P('row'), P('col')) * 3 + (P(),)
    out_specs = (weight_spec,) * 3 + (P('row'), P('col')) * 3 + (act_spec, act_spec)

    def body(w_gate, w_up, w_down, x_norm, x_act, dy_gate, dy_up, dy_down, r_gate, c_gate, r_up, c_up, r_down, c_down, hyper_params):
        m1, n1 = w_gate.shape
        m2, n2 = w_down.shape
        tokens = x_norm.shape[0]
        half = tokens // 2
        steps = half // CHUNK
        any_spec = pl.BlockSpec(memory_space=pl.ANY)
        sds = jax.ShapeDtypeStruct
        vm = pltpu.VMEM
        dma = pltpu.SemaphoreType.DMA
        outs = pl.pallas_call(
            exchange_kernel,
            name="exchange",
            out_shape=[
                sds((m1, n1), F32), sds((m1, n1), F32), sds((m2, n2), F32),
                sds((m2, n2), BF16), sds((2, tokens, n2), BF16), sds((half, m1), BF16),
                sds((m1, 128), F32), sds((m1, 128), F32), sds((m2, 128), F32),
                sds((8, 768), F32), sds((8, n1), F32), sds((8, 128), F32),
            ],
            in_specs=[any_spec] * 14 + [pl.BlockSpec(memory_space=pltpu.SMEM)],
            out_specs=[any_spec] * 12,
            scratch_shapes=[
                vm((m1, n1), F32), vm((m1, n1), F32), vm((m2, n2), F32),
                vm((m1, n1), BF16), vm((m1, n1), BF16), vm((m2, n2), BF16),
                vm((tokens, n1), BF16), vm((tokens, n1), BF16), vm((tokens, n2), BF16),
                vm((tokens, m1), BF16), vm((m1, tokens), BF16), vm((m2, tokens), BF16),
                vm((m1, n1), F32), vm((m1, n1), F32), vm((m2, n2), F32),
                vm((half, m1), F32), vm((half, m1), F32), vm((half, m1), F32), vm((half, m1), BF16),
                vm((8, 768), F32), vm((8, 768), F32), vm((8, n1), F32), vm((3, 8, n1), F32),
                vm((8, 128), F32), vm((7, 8, 128), F32),
                vm((m1,), F32), vm((n1,), F32), vm((m1,), F32), vm((n1,), F32), vm((m2,), F32), vm((n2,), F32),
                vm((m1, 128), F32), vm((m1, 128), F32), vm((m2, 128), F32),
                vm((8, 768), F32), vm((8, n1), F32), vm((8, 128), F32),
                dma((16,)), dma((12,)), dma((4,)), dma((4,)), dma((steps,)), dma((steps,)),
                dma((4,)), dma((4,)), dma((7,)), dma((7,)),
            ],
            compiler_params=pltpu.CompilerParams(
                collective_id=0, has_side_effects=True, vmem_limit_bytes=60 * 1024 * 1024
            ),
            cost_estimate=pl.CostEstimate(flops=30_000_000_000, bytes_accessed=40_000_000, transcendentals=0),
        )(w_gate, w_up, w_down, x_norm, x_act.T, dy_gate, dy_up, dy_down, r_gate, c_gate, r_up, c_up, r_down, c_down, hyper_params)
        gg, gu, gd, wd_own, dyd_all, own, rcg, rcu, rcd, rrow, crow, scal = outs
        pairs = [(0, 1), (1, 0)]
        wd_other = lax.ppermute(wd_own, 'col', pairs)
        other = lax.ppermute(own, 'col', pairs)

        def rows(*block):
            return pl.BlockSpec(block, lambda i: (i,) + (0,) * (len(block) - 1))

        def whole(*block):
            return pl.BlockSpec(block, lambda i: (0,) * len(block))

        grid = 4
        b1, b2, bt = m1 // grid, m2 // grid, tokens // grid
        wide, tall = rows(b1, n1), rows(b2, n2)
        new_gate, new_up, new_down, dx_norm, rg, cg, ru, cu, rd, cd = pl.pallas_call(
            update_kernel,
            name="update",
            grid=(grid,),
            out_shape=[
                sds((m1, n1), F32), sds((m1, n1), F32), sds((m2, n2), F32), sds((tokens, m1), BF16),
                sds((m1,), F32), sds((n1,), F32), sds((m1,), F32), sds((n1,), F32), sds((m2,), F32), sds((n2,), F32),
            ],
            in_specs=[wide, wide, tall, wide, wide, tall, rows(b1, 128), rows(b1, 128), rows(b2, 128),
                      whole(8, 768), whole(8, n1), whole(8, 128), whole(half, m1)],
            out_specs=[wide, wide, tall, any_spec,
                       whole(m1), whole(n1), whole(m1), whole(n1), whole(m2), whole(n2)],
            scratch_shapes=[dma],
            compiler_params=pltpu.CompilerParams(vmem_limit_bytes=67043328),
            cost_estimate=pl.CostEstimate(flops=3_000_000_000, bytes_accessed=14_000_000, transcendentals=0),
        )(gg, gu, gd, w_gate, w_up, w_down, rcg, rcu, rcd, rrow, crow, scal, own)

        dx_act = pl.pallas_call(
            input_grad_kernel,
            name="input_grad",
            grid=(grid,),
            out_shape=sds((m2, tokens), BF16),
            in_specs=[whole(m2, n2), whole(m2, n2), pl.BlockSpec((2, bt, n2), lambda i: (0, i, 0))],
            out_specs=pl.BlockSpec((m2, bt), lambda i: (0, i)),
            compiler_params=pltpu.CompilerParams(vmem_limit_bytes=67043328),
            cost_estimate=pl.CostEstimate(flops=4 * tokens * m2 * n2, bytes_accessed=9_000_000, transcendentals=0),
        )(wd_own, wd_other, dyd_all)

        start = (1 - lax.axis_index('col')) * half
        dx_norm = lax.dynamic_update_slice(dx_norm, other, (start, 0))
        return (new_gate, new_up, new_down, rg, cg, ru, cu, rd, cd, dx_norm, dx_act.T)

    return jax.shard_map(body, mesh=mesh, in_specs=in_specs, out_specs=out_specs, check_vma=False)
```

```python
import jax
import jax.numpy as jnp
from jax import lax
from jax.experimental import pallas as pl
from jax.experimental.pallas import tpu as pltpu
from jax.sharding import PartitionSpec as P

EPS_ONE = 1e-30
EPS_TWO = 1e-3
MESH = pl.DeviceIdType.MESH
F32 = jnp.float32
BF16 = jnp.bfloat16
NT = (((1,), (1,)), ((), ()))
CHUNK = 256
VMEM_PLAIN = 65536 * 1024 - 700 * 1024


def dot(a, b, dims=(((1,), (0,)), ((), ()))):
    return lax.dot_general(a, b, dims, preferred_element_type=F32)


def to_row(column):
    return jnp.transpose(jnp.broadcast_to(column, (column.shape[0], 128)))[0:1, :]


def to_columns(row):
    return jnp.transpose(jnp.broadcast_to(row, (128, row.shape[1])))


def exchange_kernel(
    wg, wu, wd, xn, xat, dyg, dyu, dyd, rg, cg, ru, cu, rd, cd, hp,
    gg_o, gu_o, gd_o, wd_o, wd_far, dyd_o, half_o, rcg_o, rcu_o, rcd_o, rrow_o, crow_o, scal_o,
    wg_v, wu_v, wd_v, wgb, wub, wdb, dyg_v, dyu_v, dyd_v, xn_v, xnt, xat_v, g_g, g_u, g_d,
    p_send, p_recv, p_own, half_v, rs_send, rs_recv, cs_send, cs_recv, s2_send, s2_recv,
    rg_v, cg_v, ru_v, cu_v, rd_v, cd_v, rcg_v, rcu_v, rcd_v, rrow_v, crow_v, scal_v, b_v,
    in_sem, out_sem, bulk_send, bulk_recv, p_ssem, p_rsem, st_send, st_recv, s2_ssem, s2_rsem, half_sem,
):
    c = lax.axis_index("col")
    r = lax.axis_index("row")
    rows = {0: r, 1: r + 1 - 2 * (r % 2), 2: (r + 2) % 4, 3: 3 - r}
    cols = {0: c, 1: 1 - c}
    peers = [(a, b) for a in (0, 1) for b in (0, 1, 2, 3) if (a, b) != (0, 0)]

    def peer(a, b):
        return (cols[a], rows[b])

    def remote(src, dst, ssem, rsem, who):
        return pltpu.make_async_remote_copy(
            src_ref=src, dst_ref=dst, send_sem=ssem, recv_sem=rsem, device_id=who, device_id_type=MESH
        )

    tokens = dyg.shape[0]
    half = tokens // 2
    quarter = tokens // 4
    steps = half // CHUNK
    mine, theirs = pl.multiple_of(c * half, half), pl.multiple_of((1 - c) * half, half)

    barrier = pltpu.get_barrier_semaphore()
    for a, b in peers:
        pl.semaphore_signal(barrier, inc=1, device_id=peer(a, b), device_id_type=MESH)

    loads = []

    def load(src, dst):
        copy = pltpu.make_async_copy(src, dst, in_sem.at[len(loads)])
        copy.start()
        loads.append(copy)
        return copy

    l_wg = load(wg, wg_v)
    l_wu = load(wu, wu_v)
    l_dg1 = load(dyg.at[pl.ds(theirs, half)], dyg_v.at[pl.ds(theirs, half)])
    l_du1 = load(dyu.at[pl.ds(theirs, half)], dyu_v.at[pl.ds(theirs, half)])
    l_xn = load(xn, xn_v)
    l_dg2 = load(dyg.at[pl.ds(mine, half)], dyg_v.at[pl.ds(mine, half)])
    l_du2 = load(dyu.at[pl.ds(mine, half)], dyu_v.at[pl.ds(mine, half)])
    l_xat = load(xat, xat_v)
    l_dyd = load(dyd, dyd_v)
    l_wd = load(wd, wd_v)
    l_small = [load(src, dst) for src, dst in ((rg, rg_v), (cg, cg_v), (ru, ru_v), (cu, cu_v), (rd, rd_v), (cd, cd_v))]

    pl.semaphore_wait(barrier, 7)

    my_rows = pl.ds(pl.multiple_of(r * quarter, quarter), quarter)
    f1 = remote(dyd.at[my_rows], dyd_o.at[c, my_rows], bulk_send.at[0], bulk_recv.at[0], peer(1, 0))
    f1.start()

    outs = []

    def store(src, dst):
        copy = pltpu.make_async_copy(src, dst, out_sem.at[len(outs)])
        copy.start()
        outs.append(copy)

    l_wg.wait()
    wgb[...] = wg_v[...].astype(BF16)
    l_wu.wait()
    wub[...] = wu_v[...].astype(BF16)
    l_dg1.wait()
    l_du1.wait()

    def p_copy(i):
        rows_i = pl.ds(pl.multiple_of(i * CHUNK, CHUNK), CHUNK)
        return remote(p_send.at[rows_i], p_recv.at[rows_i], p_ssem.at[i], p_rsem.at[i], peer(1, 0))

    def partial(base, i):
        rows_i = pl.ds(pl.multiple_of(base + i * CHUNK, CHUNK), CHUNK)
        return dot(dyg_v[rows_i, :], wgb[...], NT) + dot(dyu_v[rows_i, :], wub[...], NT)

    @pl.loop(0, steps // 2)
    def _(i):
        p_send[pl.ds(pl.multiple_of(i * CHUNK, CHUNK), CHUNK), :] = partial(theirs, i)
        p_copy(i).start()

    @pl.loop(steps // 2, steps)
    def _(i):
        p_send[pl.ds(pl.multiple_of(i * CHUNK, CHUNK), CHUNK), :] = partial(theirs, i)

    (m1, n1) = g_g.shape
    row_offsets, col_offsets = (0, m1, 2 * m1), (0, n1, 2 * n1)
    rs_send[...] = jnp.zeros_like(rs_send)
    l_xn.wait()

    @pl.loop(0, tokens // 256)
    def _(i):
        at = pl.ds(pl.multiple_of(i * 256, 256), 256)
        xnt[:, at] = jnp.transpose(xn_v[at, :])

    l_dg2.wait()
    l_du2.wait()

    def gradient(index, lhs, rhs, out):
        m, n = out.shape
        row_at, col_at = row_offsets[index], col_offsets[index]

        def block(lo, width, acc):
            at = pl.ds(lo, width)
            g = dot(lhs[...], rhs[:, at])
            out[:, at] = g
            sq = g * g + EPS_ONE
            cs_send[:, pl.ds(col_at + lo, width)] = jnp.sum(sq, axis=0, keepdims=True)
            for part in range(0, width, 128):
                acc = acc + sq[:, part:part + 128]
            return acc

        full = n // 256
        acc = lax.fori_loop(
            0, full, lambda i, acc: block(pl.multiple_of(i * 256, 256), 256, acc), jnp.zeros((m, 128), F32))
        if n % 256:
            acc = block(full * 256, n % 256, acc)
        rs_send[:, row_at:row_at + m] = to_row(jnp.sum(acc, axis=1, keepdims=True))

    gradient(0, xnt, dyg_v, g_g)
    gradient(1, xnt, dyu_v, g_u)
    l_xat.wait()
    l_dyd.wait()
    gradient(2, xat_v, dyd_v, g_d)

    s1_row = remote(rs_send, rs_recv, st_send.at[0], st_recv.at[0], peer(1, 0))
    s1_row.start()
    s1_col = []
    for b in (1, 2, 3):
        copy = remote(cs_send, cs_recv.at[b - 1], st_send.at[b], st_recv.at[b], peer(0, b))
        copy.start()
        s1_col.append(copy)

    @pl.loop(steps // 2, steps)
    def _(i):
        p_copy(i).start()

    def share(row, slot, who):
        at = pl.ds(pl.multiple_of(row * quarter, quarter), quarter)
        return remote(dyd_o.at[1 - c, at], dyd_o.at[1 - c, at], bulk_send.at[slot], bulk_recv.at[slot], who)

    f1.wait_recv()
    shares = [share(r, 1, peer(0, 1)), share(r, 2, peer(0, 2))]
    for copy in shares:
        copy.start()

    store(g_g, gg_o)
    store(g_u, gu_o)
    store(g_d, gd_o)
    store(dyd_v, dyd_o.at[c])

    l_wd.wait()
    wdb[...] = wd_v[...].astype(BF16)
    store(wdb, wd_o)
    f3 = remote(wdb, wd_far, bulk_send.at[4], bulk_recv.at[4], peer(1, 0))

    w_sq = [jnp.sum(jnp.sum(w[...] * w[...], axis=0, keepdims=True), axis=1, keepdims=True) for w in (wg_v, wu_v, wd_v)]

    @pl.loop(0, steps)
    def _(i):
        p_own[pl.ds(pl.multiple_of(i * CHUNK, CHUNK), CHUNK), :] = partial(mine, i)

    s1_row.wait_recv()
    for copy in s1_col:
        copy.wait_recv()
    beta = hp[0]
    for copy in l_small:
        copy.wait()
    shapes = [g.shape for g in (g_g, g_u, g_d)]
    qs, ss = [], []
    rrow_v[...] = jnp.zeros_like(rrow_v)
    crow_v[...] = jnp.ones_like(crow_v)
    for index, (g, r_ref, c_ref, rc_v) in enumerate(((g_g, rg_v, cg_v, rcg_v), (g_u, ru_v, cu_v, rcu_v), (g_d, rd_v, cd_v, rcd_v))):
        m, n = shapes[index]
        m_all, n_all = m * 4, n * 2
        row_at, col_at = pl.ds(row_offsets[index], m), pl.ds(col_offsets[index], n)
        row_sum = rs_send[:, row_at] + rs_recv[:, row_at]
        col_sum = (cs_send[:, col_at] + cs_recv[0, :, col_at]) + (cs_recv[1, :, col_at] + cs_recv[2, :, col_at])
        r_new = beta * r_ref[...].reshape(1, m) + (1.0 - beta) * (row_sum / n_all)
        c_new = beta * c_ref[...].reshape(1, n) + (1.0 - beta) * (col_sum / m_all)
        rrow_v[index:index + 1, 0:m] = r_new
        crow_v[index:index + 1, 0:n] = c_new
        q = jnp.sum(r_new, axis=1, keepdims=True) / m_all
        columns = to_columns(r_new)
        rc_v[...] = columns
        a = lax.rsqrt(columns / q)
        b_v[:, 0:n] = lax.rsqrt(c_new)

        def square(i, acc, g=g, a=a):
            at = pl.ds(pl.multiple_of(i * 128, 128), 128)
            u = g[:, at] * (a * b_v[:, at])
            return acc + u * u

        acc = lax.fori_loop(0, n // 128, square, jnp.zeros((m, 128), F32))
        qs.append(q)
        ss.append(jnp.sum(jnp.sum(acc, axis=0, keepdims=True), axis=1, keepdims=True))

    lane = lax.broadcasted_iota(jnp.int32, (1, 128), 1)

    def lanes(values, fill):
        out = jnp.full((1, 128), fill, F32)
        for index, value in enumerate(values):
            out = jnp.where(lane == index, value, out)
        return out

    s2_send[:, 0:128] = lanes(qs, 1.0)
    s2_send[:, 128:256] = lanes(ss, 0.0)
    s2_send[:, 256:384] = lanes(w_sq, 0.0)
    s2 = []
    for k, (a, b) in enumerate(peers):
        copy = remote(s2_send, s2_recv.at[k], s2_ssem.at[k], s2_rsem.at[k], peer(a, b))
        copy.start()
        s2.append(copy)

    for src, dst in ((rcg_v, rcg_o), (rcu_v, rcu_o), (rcd_v, rcd_o), (rrow_v, rrow_o), (crow_v, crow_o)):
        store(src, dst)

    def half_copy(i):
        rows_i = pl.ds(pl.multiple_of(i * CHUNK, CHUNK), CHUNK)
        return pltpu.make_async_copy(half_v.at[rows_i], half_o.at[rows_i], half_sem.at[i])

    shares[1].wait_recv()
    relay = share(rows[2], 3, peer(0, 1))
    relay.start()
    shares.append(relay)

    @pl.when(r % 2 == 1)
    def _():
        f3.start()

    @pl.loop(0, steps)
    def _(i):
        rows_i = pl.ds(pl.multiple_of(i * CHUNK, CHUNK), CHUNK)
        p_copy(i).wait_recv()
        half_v[rows_i, :] = (p_own[rows_i, :] + p_recv[rows_i, :]).astype(BF16)
        half_copy(i).start()

    for copy in s2:
        copy.wait_recv()
    table = [s2_send[...]] + [s2_recv[k] for k in range(7)]

    def tree(values):
        while len(values) > 1:
            values = [values[k] + values[k + 1] for k in range(0, len(values), 2)]
        return values[0]

    r_mean = tree([t[:, 0:128] for t in table[:4]])
    u_sq = []
    for t in table:
        ratio = jnp.sqrt(r_mean) / jnp.sqrt(t[:, 0:128])
        u_sq.append((t[:, 128:256] * ratio) * ratio)
    size = F32(shapes[0][0] * shapes[0][1] * 8)
    rms_u = jnp.sqrt(tree(u_sq) / size)
    step_size = hp[1] * jnp.maximum(EPS_TWO, jnp.sqrt(tree([t[:, 256:384] for t in table]) / size))
    scal_v[...] = jnp.zeros_like(scal_v)
    scal_v[0:1, :] = r_mean
    scal_v[1:2, :] = 1.0 / jnp.maximum(1.0, rms_u / hp[2])
    scal_v[2:3, :] = step_size
    store(scal_v, scal_o)

    for copy in (shares[0], relay):
        copy.wait_recv()
    @pl.when(r % 2 == 1)
    def _():
        f3.wait()

    for copy in [f1, s1_row] + s1_col + shares + s2:
        copy.wait_send()

    @pl.loop(0, steps)
    def _(i):
        p_copy(i).wait_send()
        half_copy(i).wait()

    for copy in outs:
        copy.wait()


def update_kernel(
    gg, gu, gd, wg, wu, wd, rcg, rcu, rcd, rrow, crow, scal,
    wg_o, wu_o, wd_o, rg_o, cg_o, ru_o, cu_o, rd_o, cd_o,
):
    @pl.when(pl.program_id(0) == 0)
    def _():
        for index, (r_out, c_out) in enumerate(((rg_o, cg_o), (ru_o, cu_o), (rd_o, cd_o))):
            r_out[...] = rrow[index:index + 1, 0:r_out.shape[0]].reshape(r_out.shape)
            c_out[...] = crow[index:index + 1, 0:c_out.shape[0]].reshape(c_out.shape)

    for index, (g, w, rc, out) in enumerate(((gg, wg, rcg, wg_o), (gu, wu, rcu, wu_o), (gd, wd, rcd, wd_o))):
        n = g.shape[1]
        r_mean = scal[0:1, index:index + 1]
        inv = scal[1:2, index:index + 1]
        step = scal[2:3, index:index + 1]
        a = lax.rsqrt(rc[...] / r_mean)
        b_row = lax.rsqrt(crow[index:index + 1, 0:n])
        for lo in range(0, n, 128):
            u = g[:, lo:lo + 128] * (a * b_row[:, lo:lo + 128])
            out[:, lo:lo + 128] = w[:, lo:lo + 128] - step * (u * inv)


def input_grad_kernel(
    wd_own, wd_near, wd_far, own, dyd_all, dx_o, dxn_o, wd_all, dyd_v, dx_v, own_v, wd_sem, own_sem, dyd_sem, dx_sem,
):
    c = lax.axis_index("col")
    odd = lax.axis_index("row") % 2 == 1
    half = own.shape[0]
    count = dyd_v.shape[1] // CHUNK

    def tokens(i):
        return pl.ds(pl.multiple_of(i * CHUNK, CHUNK), CHUNK)

    def dyd_copy(i):
        return pltpu.make_async_copy(dyd_all.at[:, tokens(i)], dyd_v.at[:, tokens(i)], dyd_sem.at[i])

    def dx_copy(i):
        return pltpu.make_async_copy(dx_v.at[:, tokens(i)], dx_o.at[:, tokens(i)], dx_sem.at[i])

    mine = pltpu.make_async_copy(wd_own, wd_all.at[c], wd_sem.at[0])
    near = pltpu.make_async_copy(wd_near, wd_all.at[1 - c], wd_sem.at[1])
    far = pltpu.make_async_copy(wd_far, wd_all.at[1 - c], wd_sem.at[1])
    take = pltpu.make_async_copy(own, own_v, own_sem.at[0])
    place = pltpu.make_async_copy(own_v, dxn_o.at[pl.ds(pl.multiple_of(c * half, half), half)], own_sem.at[1])
    dyd_copy(0).start()
    mine.start()
    pl.when(odd)(near.start)
    pl.when(jnp.logical_not(odd))(far.start)
    dyd_copy(1).start()
    dyd_copy(2).start()
    take.start()

    @pl.loop(3, count)
    def _(i):
        dyd_copy(i).start()

    mine.wait()
    far.wait()

    @pl.loop(0, count)
    def _(i):
        dyd_copy(i).wait()
        dx = dot(wd_all[0], dyd_v[0, tokens(i), :], NT) + dot(wd_all[1], dyd_v[1, tokens(i), :], NT)
        dx_v[:, tokens(i)] = dx.astype(BF16)
        dx_copy(i).start()

        @pl.when(i == 2)
        def _():
            take.wait()
            place.start()

    place.wait()

    @pl.loop(0, count)
    def _(i):
        dx_copy(i).wait()


def solution(mesh):
    weight_spec = P('row', 'col')
    act_spec = P(None, 'row')
    grad_spec = P(None, 'col')
    in_specs = (weight_spec,) * 3 + (act_spec, act_spec) + (grad_spec,) * 3 + (P('row'), P('col')) * 3 + (P(),)
    out_specs = (weight_spec,) * 3 + (P('row'), P('col')) * 3 + (act_spec, act_spec)

    def body(w_gate, w_up, w_down, x_norm, x_act, dy_gate, dy_up, dy_down, r_gate, c_gate, r_up, c_up, r_down, c_down, hyper_params):
        m1, n1 = w_gate.shape
        m2, n2 = w_down.shape
        tokens = x_norm.shape[0]
        half = tokens // 2
        steps = half // CHUNK
        row_len, col_len = 2 * m1 + 768, 2 * n1 + n2
        any_spec = pl.BlockSpec(memory_space=pl.ANY)
        sds = jax.ShapeDtypeStruct
        vm = pltpu.VMEM
        dma = pltpu.SemaphoreType.DMA
        outs = pl.pallas_call(
            exchange_kernel,
            name="exchange",
            out_shape=[
                sds((m1, n1), F32), sds((m1, n1), F32), sds((m2, n2), F32),
                sds((m2, n2), BF16), sds((m2, n2), BF16), sds((2, tokens, n2), BF16), sds((half, m1), BF16),
                sds((m1, 128), F32), sds((m1, 128), F32), sds((m2, 128), F32),
                sds((8, 768), F32), sds((8, n1), F32), sds((8, 128), F32),
            ],
            in_specs=[any_spec] * 14 + [pl.BlockSpec(memory_space=pltpu.SMEM)],
            out_specs=[any_spec] * 13,
            scratch_shapes=[
                vm((m1, n1), F32), vm((m1, n1), F32), vm((m2, n2), F32),
                vm((m1, n1), BF16), vm((m1, n1), BF16), vm((m2, n2), BF16),
                vm((tokens, n1), BF16), vm((tokens, n1), BF16), vm((tokens, n2), BF16),
                vm((tokens, m1), BF16), vm((m1, tokens), BF16), vm((m2, tokens), BF16),
                vm((m1, n1), F32), vm((m1, n1), F32), vm((m2, n2), F32),
                vm((half, m1), F32), vm((half, m1), F32), vm((half, m1), F32), vm((half, m1), BF16),
                vm((1, row_len), F32), vm((1, row_len), F32), vm((1, col_len), F32), vm((3, 1, col_len), F32),
                vm((1, 384), F32), vm((7, 1, 384), F32),
                vm((m1,), F32), vm((n1,), F32), vm((m1,), F32), vm((n1,), F32), vm((m2,), F32), vm((n2,), F32),
                vm((m1, 128), F32), vm((m1, 128), F32), vm((m2, 128), F32),
                vm((8, 768), F32), vm((8, n1), F32), vm((8, 128), F32), vm((1, n1), F32),
                dma((16,)), dma((12,)), dma((5,)), dma((5,)), dma((steps,)), dma((steps,)),
                dma((4,)), dma((4,)), dma((7,)), dma((7,)), dma((steps,)),
            ],
            compiler_params=pltpu.CompilerParams(
                collective_id=0, has_side_effects=True, vmem_limit_bytes=60 * 1024 * 1024
            ),
            cost_estimate=pl.CostEstimate(flops=30_000_000_000, bytes_accessed=40_000_000, transcendentals=0),
        )(w_gate, w_up, w_down, x_norm, x_act.T, dy_gate, dy_up, dy_down, r_gate, c_gate, r_up, c_up, r_down, c_down, hyper_params)
        gg, gu, gd, wd_own, wd_near, dyd_all, own, rcg, rcu, rcd, rrow, crow, scal = outs
        pairs = [(0, 1), (1, 0)]
        even = [(0, 4), (4, 0), (2, 6), (6, 2)]
        wd_far = lax.ppermute(wd_own, ('col', 'row'), even)
        other = lax.ppermute(own, 'col', pairs)

        def rows(*block):
            return pl.BlockSpec(block, lambda i: (i,) + (0,) * (len(block) - 1))

        def whole(*block):
            return pl.BlockSpec(block, lambda i: (0,) * len(block))

        grid = 4
        b1, b2, bt = m1 // grid, m2 // grid, tokens // grid
        wide, tall = rows(b1, n1), rows(b2, n2)
        new_gate, new_up, new_down, rg, cg, ru, cu, rd, cd = pl.pallas_call(
            update_kernel,
            name="update",
            grid=(grid,),
            out_shape=[
                sds((m1, n1), F32), sds((m1, n1), F32), sds((m2, n2), F32),
                sds((m1,), F32), sds((n1,), F32), sds((m1,), F32), sds((n1,), F32), sds((m2,), F32), sds((n2,), F32),
            ],
            in_specs=[wide, wide, tall, wide, wide, tall, rows(b1, 128), rows(b1, 128), rows(b2, 128),
                      whole(8, 768), whole(8, n1), whole(8, 128)],
            out_specs=[wide, wide, tall,
                       whole(m1), whole(n1), whole(m1), whole(n1), whole(m2), whole(n2)],
            compiler_params=pltpu.CompilerParams(vmem_limit_bytes=VMEM_PLAIN),
            cost_estimate=pl.CostEstimate(flops=3_000_000_000, bytes_accessed=14_000_000, transcendentals=0),
        )(gg, gu, gd, w_gate, w_up, w_down, rcg, rcu, rcd, rrow, crow, scal)

        dx_act, dx_norm = pl.pallas_call(
            input_grad_kernel,
            name="input_grad",
            out_shape=[sds((m2, tokens), BF16), sds((tokens, m1), BF16)],
            in_specs=[any_spec] * 5,
            out_specs=[any_spec] * 2,
            scratch_shapes=[
                vm((2, m2, n2), BF16), vm((2, tokens, n2), BF16), vm((m2, tokens), BF16), vm((half, m1), BF16),
                dma((2,)), dma((2,)), dma((tokens // CHUNK,)), dma((tokens // CHUNK,)),
            ],
            compiler_params=pltpu.CompilerParams(vmem_limit_bytes=VMEM_PLAIN),
            cost_estimate=pl.CostEstimate(flops=4 * tokens * m2 * n2, bytes_accessed=9_000_000, transcendentals=0),
        )(wd_own, wd_near, wd_far, own, dyd_all)

        start = (1 - lax.axis_index('col')) * half
        dx_norm = lax.dynamic_update_slice(dx_norm, other, (start, 0))
        return (new_gate, new_up, new_down, rg, cg, ru, cu, rd, cd, dx_norm, dx_act.T)

    return jax.shard_map(body, mesh=mesh, in_specs=in_specs, out_specs=out_specs, check_vma=False)
```

```python
import jax
import jax.numpy as jnp
from jax import lax
from jax.experimental import pallas as pl
from jax.experimental.pallas import tpu as pltpu
from jax.sharding import PartitionSpec as P

EPS_ONE = 1e-30
EPS_TWO = 1e-3
MESH = pl.DeviceIdType.MESH
F32 = jnp.float32
BF16 = jnp.bfloat16
NT = (((1,), (1,)), ((), ()))
CHUNK = 256
LATE = 1
EARLY_EIGHTHS = 2
VMEM_PLAIN = 65536 * 1024 - 700 * 1024


def dot(a, b, dims=(((1,), (0,)), ((), ()))):
    return lax.dot_general(a, b, dims, preferred_element_type=F32)


def to_row(column):
    return jnp.transpose(jnp.broadcast_to(column, (column.shape[0], 128)))[0:1, :]


def to_columns(row):
    return jnp.transpose(jnp.broadcast_to(row, (128, row.shape[1])))


def exchange_kernel(
    wg, wu, wd, xn, xat, dyg, dyu, dyd, rg, cg, ru, cu, rd, cd, hyper,
    gg_o, gu_o, gd_o, wd_o, wd_far, dyd_o, half_o, rcg_o, rcu_o, rcd_o, rrow_o, crow_o, scal_o,
    wg_v, wu_v, wd_v, wgb, wub, wdb, dyg_v, dyu_v, dyd_v, xn_v, xnt, xat_v, g_g, g_u, g_d,
    p_send, p_recv, p_own, half_v, rs_send, rs_recv, cs_send, cs_recv, s2_send, s2_recv, tot_send, tot_recv,
    rg_v, cg_v, ru_v, cu_v, rd_v, cd_v, rcg_v, rcu_v, rcd_v, rrow_v, crow_v, scal_v, b_v, hp,
    in_sem, out_sem, bulk_send, bulk_recv, p_ssem, p_rsem, st_send, st_recv, s2_ssem, s2_rsem, half_sem,
):
    c = lax.axis_index("col")
    r = lax.axis_index("row")
    rows = {0: r, 1: r + 1 - 2 * (r % 2), 2: (r + 2) % 4, 3: 3 - r}
    cols = {0: c, 1: 1 - c}
    peers = [(1, 0), (0, 1), (0, 2), (0, 3)]

    def peer(a, b):
        return (cols[a], rows[b])

    def remote(src, dst, ssem, rsem, who):
        return pltpu.make_async_remote_copy(
            src_ref=src, dst_ref=dst, send_sem=ssem, recv_sem=rsem, device_id=who, device_id_type=MESH
        )

    tokens = dyg.shape[0]
    half = tokens // 2
    steps = half // CHUNK
    mine, theirs = pl.multiple_of(c * half, half), pl.multiple_of((1 - c) * half, half)

    barrier = pltpu.get_barrier_semaphore()
    for a, b in peers:
        pl.semaphore_signal(barrier, inc=1, device_id=peer(a, b), device_id_type=MESH)

    loads = []

    def load(src, dst):
        copy = pltpu.make_async_copy(src, dst, in_sem.at[len(loads)])
        copy.start()
        loads.append(copy)
        return copy

    l_dyd = load(dyd, dyd_v)
    l_wg = load(wg, wg_v)
    l_wu = load(wu, wu_v)
    l_dg1 = load(dyg.at[pl.ds(theirs, half)], dyg_v.at[pl.ds(theirs, half)])
    l_du1 = load(dyu.at[pl.ds(theirs, half)], dyu_v.at[pl.ds(theirs, half)])
    l_xn = load(xn, xn_v)
    l_dg2 = load(dyg.at[pl.ds(mine, half)], dyg_v.at[pl.ds(mine, half)])
    l_du2 = load(dyu.at[pl.ds(mine, half)], dyu_v.at[pl.ds(mine, half)])
    l_xat = load(xat, xat_v)
    l_wd = load(wd, wd_v)
    l_small = [load(src, dst) for src, dst in ((rg, rg_v), (cg, cg_v), (ru, ru_v), (cu, cu_v), (rd, rd_v), (cd, cd_v), (hyper, hp))]

    pl.semaphore_wait(barrier, len(peers))

    few = half * EARLY_EIGHTHS // 8

    def part(x, core):
        start, size = (few, half - few) if core == LATE else (0, few)
        return pl.ds(pl.multiple_of(x * half + start, 128), size)

    def f1(core):
        at = part(r // 2, core)
        return remote(dyd_v.at[at], dyd_o.at[c, at], bulk_send.at[0], bulk_recv.at[0], peer(1, 0))

    def share(x, core, slot, who):
        at = part(x, core)
        return remote(dyd_o.at[1 - c, at], dyd_o.at[1 - c, at], bulk_send.at[slot], bulk_recv.at[slot], who)

    def on_core(body):
        for core in (0, 1):
            pl.when(r % 2 == core)(lambda core=core: body(core))

    near_x, far_x = r // 2, 1 - r // 2
    l_dyd.wait()
    on_core(lambda core: f1(core).start())

    outs = []

    def store(src, dst):
        copy = pltpu.make_async_copy(src, dst, out_sem.at[len(outs)])
        copy.start()
        outs.append(copy)

    l_wg.wait()
    wgb[...] = wg_v[...].astype(BF16)
    l_wu.wait()
    wub[...] = wu_v[...].astype(BF16)
    l_dg1.wait()
    l_du1.wait()

    def p_copy(i):
        rows_i = pl.ds(pl.multiple_of(i * CHUNK, CHUNK), CHUNK)
        return remote(p_send.at[rows_i], p_recv.at[rows_i], p_ssem.at[i], p_rsem.at[i], peer(1, 0))

    def partial(base, i):
        rows_i = pl.ds(pl.multiple_of(base + i * CHUNK, CHUNK), CHUNK)
        return dot(dyg_v[rows_i, :], wgb[...], NT) + dot(dyu_v[rows_i, :], wub[...], NT)

    @pl.loop(0, steps // 2)
    def _(i):
        p_send[pl.ds(pl.multiple_of(i * CHUNK, CHUNK), CHUNK), :] = partial(theirs, i)
        pl.when(r % 2 != LATE)(lambda: p_copy(i).start())

    @pl.loop(steps // 2, steps)
    def _(i):
        p_send[pl.ds(pl.multiple_of(i * CHUNK, CHUNK), CHUNK), :] = partial(theirs, i)

    (m1, n1) = g_g.shape
    row_offsets, col_offsets = (0, m1, 2 * m1), (0, n1, 2 * n1)
    rs_send[...] = jnp.zeros_like(rs_send)
    l_xn.wait()

    @pl.loop(0, tokens // 256)
    def _(i):
        at = pl.ds(pl.multiple_of(i * 256, 256), 256)
        xnt[:, at] = jnp.transpose(xn_v[at, :])

    l_dg2.wait()
    l_du2.wait()

    def gradient(index, lhs, rhs, out):
        m, n = out.shape
        row_at, col_at = row_offsets[index], col_offsets[index]

        def block(lo, width, acc):
            at = pl.ds(lo, width)
            g = dot(lhs[...], rhs[:, at])
            out[:, at] = g
            sq = g * g + EPS_ONE
            cs_send[:, pl.ds(col_at + lo, width)] = jnp.sum(sq, axis=0, keepdims=True)
            for part in range(0, width, 128):
                acc = acc + sq[:, part:part + 128]
            return acc

        full = n // 256
        acc = lax.fori_loop(
            0, full, lambda i, acc: block(pl.multiple_of(i * 256, 256), 256, acc), jnp.zeros((m, 128), F32))
        if n % 256:
            acc = block(full * 256, n % 256, acc)
        rs_send[:, row_at:row_at + m] = to_row(jnp.sum(acc, axis=1, keepdims=True))

    gradient(0, xnt, dyg_v, g_g)
    gradient(1, xnt, dyu_v, g_u)
    l_xat.wait()
    gradient(2, xat_v, dyd_v, g_d)

    s1_row = remote(rs_send, rs_recv, st_send.at[0], st_recv.at[0], peer(1, 0))
    s1_row.start()
    s1_col = []
    for b in (1, 2, 3):
        copy = remote(cs_send, cs_recv.at[b - 1], st_send.at[b], st_recv.at[b], peer(0, b))
        copy.start()
        s1_col.append(copy)

    @pl.when(r % 2 == LATE)
    def _():
        @pl.loop(0, steps // 2)
        def _(i):
            p_copy(i).start()

    @pl.loop(steps // 2, steps)
    def _(i):
        p_copy(i).start()

    store(g_g, gg_o)
    store(g_u, gu_o)
    store(g_d, gd_o)
    store(dyd_v, dyd_o.at[c])

    l_wd.wait()
    wdb[...] = wd_v[...].astype(BF16)
    store(wdb, wd_o)
    f3 = remote(wdb, wd_far, bulk_send.at[4], bulk_recv.at[4], peer(1, 0))

    @pl.when(r % 2 == LATE)
    def _():
        f3.start()


    w_sq = [jnp.sum(jnp.sum(w[...] * w[...], axis=0, keepdims=True), axis=1, keepdims=True) for w in (wg_v, wu_v, wd_v)]

    @pl.loop(0, steps)
    def _(i):
        p_own[pl.ds(pl.multiple_of(i * CHUNK, CHUNK), CHUNK), :] = partial(mine, i)

    @on_core
    def _(core):
        f1(core).wait()
        share(near_x, core, 1, peer(0, 1)).start()
        share(near_x, core, 2, peer(0, 2)).start()

    s1_row.wait_recv()
    for copy in s1_col:
        copy.wait_recv()
    for copy in l_small:
        copy.wait()
    beta = hp[0]
    shapes = [g.shape for g in (g_g, g_u, g_d)]
    qs, ss = [], []
    rrow_v[...] = jnp.zeros_like(rrow_v)
    crow_v[...] = jnp.ones_like(crow_v)
    for index, (g, r_ref, c_ref, rc_v) in enumerate(((g_g, rg_v, cg_v, rcg_v), (g_u, ru_v, cu_v, rcu_v), (g_d, rd_v, cd_v, rcd_v))):
        m, n = shapes[index]
        m_all, n_all = m * 4, n * 2
        row_at, col_at = pl.ds(row_offsets[index], m), pl.ds(col_offsets[index], n)
        row_sum = rs_send[:, row_at] + rs_recv[:, row_at]
        col_sum = (cs_send[:, col_at] + cs_recv[0, :, col_at]) + (cs_recv[1, :, col_at] + cs_recv[2, :, col_at])
        r_new = beta * r_ref[...].reshape(1, m) + (1.0 - beta) * (row_sum / n_all)
        c_new = beta * c_ref[...].reshape(1, n) + (1.0 - beta) * (col_sum / m_all)
        rrow_v[index:index + 1, 0:m] = r_new
        crow_v[index:index + 1, 0:n] = c_new
        q = jnp.sum(r_new, axis=1, keepdims=True) / m_all
        columns = to_columns(r_new)
        rc_v[...] = columns
        a = lax.rsqrt(columns / q)
        b_v[:, 0:n] = lax.rsqrt(c_new)

        def square(i, acc, g=g, a=a):
            at = pl.ds(pl.multiple_of(i * 128, 128), 128)
            u = g[:, at] * (a * b_v[:, at])
            return acc + u * u

        acc = lax.fori_loop(0, n // 128, square, jnp.zeros((m, 128), F32))
        qs.append(q)
        ss.append(jnp.sum(jnp.sum(acc, axis=0, keepdims=True), axis=1, keepdims=True))

    lane = lax.broadcasted_iota(jnp.int32, (1, 128), 1)

    def lanes(values, fill):
        out = jnp.full((1, 128), fill, F32)
        for index, value in enumerate(values):
            out = jnp.where(lane == index, value, out)
        return out

    s2_send[:, 0:128] = lanes(qs, 1.0)
    s2_send[:, 128:256] = lanes(ss, 0.0)
    s2_send[:, 256:384] = lanes(w_sq, 0.0)
    s2 = []
    for b in (1, 2, 3):
        copy = remote(s2_send, s2_recv.at[b - 1], s2_ssem.at[b - 1], s2_rsem.at[b - 1], peer(0, b))
        copy.start()
        s2.append(copy)

    for src, dst in ((rcg_v, rcg_o), (rcu_v, rcu_o), (rcd_v, rcd_o), (rrow_v, rrow_o), (crow_v, crow_o)):
        store(src, dst)

    def half_copy(i):
        rows_i = pl.ds(pl.multiple_of(i * CHUNK, CHUNK), CHUNK)
        return pltpu.make_async_copy(half_v.at[rows_i], half_o.at[rows_i], half_sem.at[i])

    @on_core
    def _(core):
        share(far_x, core, 2, peer(0, 2)).wait_recv()
        share(far_x, core, 3, peer(0, 1)).start()

    for copy in s2:
        copy.wait_recv()
    table = [s2_send[...]] + [s2_recv[k] for k in range(3)]

    def tree(values):
        return (values[0] + values[1]) + (values[2] + values[3])

    r_mean = tree([t[:, 0:128] for t in table])
    u_sq = []
    for t in table:
        ratio = jnp.sqrt(r_mean) / jnp.sqrt(t[:, 0:128])
        u_sq.append((t[:, 128:256] * ratio) * ratio)
    tot_send[:, 0:128] = tree(u_sq)
    tot_send[:, 128:256] = tree([t[:, 256:384] for t in table])

    tot_copy = remote(tot_send, tot_recv, s2_ssem.at[3], s2_rsem.at[3], peer(1, 0))
    tot_tell = remote(tot_recv, tot_recv, s2_ssem.at[4], s2_rsem.at[4], peer(0, 1))

    @pl.when(r % 2 != LATE)
    def _():
        tot_copy.start()

    @pl.loop(0, steps)
    def _(i):
        rows_i = pl.ds(pl.multiple_of(i * CHUNK, CHUNK), CHUNK)
        p_copy(i).wait_recv()
        half_v[rows_i, :] = (p_own[rows_i, :] + p_recv[rows_i, :]).astype(BF16)
        half_copy(i).start()

    @pl.when(r % 2 != LATE)
    def _():
        tot_copy.wait()
        tot_tell.start()

    @pl.when(r % 2 == LATE)
    def _():
        tot_tell.wait_recv()

    total = tot_send[...] + tot_recv[...]
    size = F32(shapes[0][0] * shapes[0][1] * 8)
    rms_u = jnp.sqrt(total[:, 0:128] / size)
    step_size = hp[1] * jnp.maximum(EPS_TWO, jnp.sqrt(total[:, 128:256] / size))
    scal_v[...] = jnp.zeros_like(scal_v)
    scal_v[0:1, :] = r_mean
    scal_v[1:2, :] = 1.0 / jnp.maximum(1.0, rms_u / hp[2])
    scal_v[2:3, :] = step_size
    store(scal_v, scal_o)


    @on_core
    def _(core):
        share(near_x, 1 - core, 1, peer(0, 1)).wait_recv()
        share(far_x, 1 - core, 3, peer(0, 1)).wait_recv()
        share(near_x, core, 1, peer(0, 1)).wait_send()
        share(near_x, core, 2, peer(0, 2)).wait_send()
        share(far_x, core, 3, peer(0, 1)).wait_send()

    @pl.when(r % 2 == LATE)
    def _():
        f3.wait()

    @pl.when(r % 2 != LATE)
    def _():
        tot_tell.wait_send()

    for copy in [s1_row] + s1_col + s2:
        copy.wait_send()

    @pl.loop(0, steps)
    def _(i):
        p_copy(i).wait_send()
        half_copy(i).wait()

    for copy in outs:
        copy.wait()


def token_rows(i):
    return pl.ds(pl.multiple_of(i * CHUNK, CHUNK), CHUNK)


class InputGrad:
    def __init__(self, wd_own, wd_other, dyd_all, dx_o, wd_all, dyd_v, dx_v, wd_sem, dyd_sem, dx_sem):
        c = lax.axis_index("col")
        self.count = dyd_v.shape[1] // CHUNK
        self.weights = [
            pltpu.make_async_copy(wd_own, wd_all.at[c], wd_sem.at[0]),
            pltpu.make_async_copy(wd_other, wd_all.at[1 - c], wd_sem.at[1]),
        ]
        self.refs = wd_all, dyd_all, dyd_v, dx_v, dx_o, dyd_sem, dx_sem

    def dyd_copy(self, i):
        wd_all, dyd_all, dyd_v, dx_v, dx_o, dyd_sem, dx_sem = self.refs
        return pltpu.make_async_copy(dyd_all.at[:, token_rows(i)], dyd_v.at[:, token_rows(i)], dyd_sem.at[i])

    def dx_copy(self, i):
        wd_all, dyd_all, dyd_v, dx_v, dx_o, dyd_sem, dx_sem = self.refs
        return pltpu.make_async_copy(dx_v.at[:, token_rows(i)], dx_o.at[:, token_rows(i)], dx_sem.at[i])

    def fetch(self, lo, hi):
        @pl.loop(lo, hi)
        def _(i):
            self.dyd_copy(i).start()

    def multiply(self, lo, hi):
        wd_all, dyd_all, dyd_v, dx_v, dx_o, dyd_sem, dx_sem = self.refs

        @pl.loop(lo, hi)
        def _(i):
            self.dyd_copy(i).wait()
            dx = dot(wd_all[0], dyd_v[0, token_rows(i), :], NT) + dot(wd_all[1], dyd_v[1, token_rows(i), :], NT)
            dx_v[:, token_rows(i)] = dx.astype(BF16)
            self.dx_copy(i).start()

    def finish(self):
        @pl.loop(0, self.count)
        def _(i):
            self.dx_copy(i).wait()


def update_kernel(
    gg, gu, gd, wg, wu, wd, rcg, rcu, rcd, rrow, crow, scal, own, wd_own, wd_near, dyd_all,
    wg_o, wu_o, wd_o, dx_o, dxn_o, rg_o, cg_o, ru_o, cu_o, rd_o, cd_o,
    gg_v, gu_v, gd_v, wg_v, wu_v, wd_v, rcg_v, rcu_v, rcd_v, rrow_v, crow_v, scal_v, own_v, wd_all, dyd_v, dx_v,
    rg_v, cg_v, ru_v, cu_v, rd_v, cd_v, in_sem, out_sem, wd_sem, dyd_sem, dx_sem,
):
    c = lax.axis_index("col")
    late = lax.axis_index("row") % 2 == LATE
    half = own.shape[0]
    grad = InputGrad(wd_own, wd_near, dyd_all, dx_o, wd_all, dyd_v, dx_v, wd_sem, dyd_sem, dx_sem)
    loads, outs = [], []

    def load(src, dst):
        copy = pltpu.make_async_copy(src, dst, in_sem.at[len(loads)])
        loads.append(copy)
        copy.start()
        return copy

    def store(src, dst):
        copy = pltpu.make_async_copy(src, dst, out_sem.at[len(outs)])
        outs.append(copy)
        copy.start()

    l_gg, l_wg = load(gg, gg_v), load(wg, wg_v)
    l_small = [load(rcg, rcg_v), load(rcu, rcu_v), load(rcd, rcd_v), load(rrow, rrow_v), load(crow, crow_v), load(scal, scal_v)]

    @pl.when(late)
    def _():
        for copy in grad.weights:
            copy.start()
        grad.fetch(0, 3)

    l_gu, l_wu = load(gu, gu_v), load(wu, wu_v)

    @pl.when(late)
    def _():
        grad.fetch(3, 6)

    l_gd, l_wd = load(gd, gd_v), load(wd, wd_v)
    l_own = load(own, own_v)

    @pl.when(late)
    def _():
        grad.fetch(6, grad.count)

    def update(index, waits, g, w, rc, out):
        for copy in waits:
            copy.wait()
        n = g.shape[1]
        r_mean = scal_v[0:1, index:index + 1]
        inv = scal_v[1:2, index:index + 1]
        step = scal_v[2:3, index:index + 1]
        a = lax.rsqrt(rc[...] / r_mean)
        b_row = lax.rsqrt(crow_v[index:index + 1, 0:n])
        for lo in range(0, n, 128):
            u = g[:, lo:lo + 128] * (a * b_row[:, lo:lo + 128])
            w[:, lo:lo + 128] = w[:, lo:lo + 128] - step * (u * inv)
        store(w, out)

    for copy in l_small:
        copy.wait()
    update(0, (l_gg, l_wg), gg_v, wg_v, rcg_v, wg_o)
    for index, (r_v, c_v, r_out, c_out) in enumerate(
            ((rg_v, cg_v, rg_o, cg_o), (ru_v, cu_v, ru_o, cu_o), (rd_v, cd_v, rd_o, cd_o))):
        r_v[...] = rrow_v[index:index + 1, 0:r_v.shape[0]].reshape(r_v.shape)
        c_v[...] = crow_v[index:index + 1, 0:c_v.shape[0]].reshape(c_v.shape)
        store(r_v, r_out)
        store(c_v, c_out)

    @pl.when(late)
    def _():
        for copy in grad.weights:
            copy.wait()
        grad.multiply(0, 3)

    update(1, (l_gu, l_wu), gu_v, wu_v, rcu_v, wu_o)

    @pl.when(late)
    def _():
        grad.multiply(3, 6)

    update(2, (l_gd, l_wd), gd_v, wd_v, rcd_v, wd_o)
    l_own.wait()
    store(own_v, dxn_o.at[pl.ds(pl.multiple_of(c * half, half), half)])

    @pl.when(late)
    def _():
        grad.multiply(6, grad.count)
        grad.finish()

    for copy in outs:
        copy.wait()


def input_grad_kernel(
    wd_own, wd_far, dyd_all, dx_in, dxn_in, dx_o, dxn_o, wd_all, dyd_v, dx_v, wd_sem, dyd_sem, dx_sem,
):
    grad = InputGrad(wd_own, wd_far, dyd_all, dx_o, wd_all, dyd_v, dx_v, wd_sem, dyd_sem, dx_sem)

    @pl.when(lax.axis_index("row") % 2 != LATE)
    def _():
        grad.fetch(0, 1)
        for copy in grad.weights:
            copy.start()
        grad.fetch(1, grad.count)
        for copy in grad.weights:
            copy.wait()
        grad.multiply(0, grad.count)
        grad.finish()


def solution(mesh):
    weight_spec = P('row', 'col')
    act_spec = P(None, 'row')
    grad_spec = P(None, 'col')
    in_specs = (weight_spec,) * 3 + (act_spec, act_spec) + (grad_spec,) * 3 + (P('row'), P('col')) * 3 + (P(),)
    out_specs = (weight_spec,) * 3 + (P('row'), P('col')) * 3 + (act_spec, act_spec)

    def body(w_gate, w_up, w_down, x_norm, x_act, dy_gate, dy_up, dy_down, r_gate, c_gate, r_up, c_up, r_down, c_down, hyper_params):
        m1, n1 = w_gate.shape
        m2, n2 = w_down.shape
        tokens = x_norm.shape[0]
        half = tokens // 2
        steps = half // CHUNK
        row_len, col_len = 2 * m1 + 768, 2 * n1 + n2
        any_spec = pl.BlockSpec(memory_space=pl.ANY)
        sds = jax.ShapeDtypeStruct
        vm = pltpu.VMEM
        dma = pltpu.SemaphoreType.DMA
        outs = pl.pallas_call(
            exchange_kernel,
            name="exchange",
            out_shape=[
                sds((m1, n1), F32), sds((m1, n1), F32), sds((m2, n2), F32),
                sds((m2, n2), BF16), sds((m2, n2), BF16), sds((2, tokens, n2), BF16), sds((half, m1), BF16),
                sds((m1, 128), F32), sds((m1, 128), F32), sds((m2, 128), F32),
                sds((8, 768), F32), sds((8, n1), F32), sds((8, 128), F32),
            ],
            in_specs=[any_spec] * 15,
            out_specs=[any_spec] * 13,
            scratch_shapes=[
                vm((m1, n1), F32), vm((m1, n1), F32), vm((m2, n2), F32),
                vm((m1, n1), BF16), vm((m1, n1), BF16), vm((m2, n2), BF16),
                vm((tokens, n1), BF16), vm((tokens, n1), BF16), vm((tokens, n2), BF16),
                vm((tokens, m1), BF16), vm((m1, tokens), BF16), vm((m2, tokens), BF16),
                vm((m1, n1), F32), vm((m1, n1), F32), vm((m2, n2), F32),
                vm((half, m1), F32), vm((half, m1), F32), vm((half, m1), F32), vm((half, m1), BF16),
                vm((1, row_len), F32), vm((1, row_len), F32), vm((1, col_len), F32), vm((3, 1, col_len), F32),
                vm((1, 384), F32), vm((3, 1, 384), F32), vm((1, 256), F32), vm((1, 256), F32),
                vm((m1,), F32), vm((n1,), F32), vm((m1,), F32), vm((n1,), F32), vm((m2,), F32), vm((n2,), F32),
                vm((m1, 128), F32), vm((m1, 128), F32), vm((m2, 128), F32),
                vm((8, 768), F32), vm((8, n1), F32), vm((8, 128), F32), vm((1, n1), F32), pltpu.SMEM((3,), F32),
                dma((17,)), dma((12,)), dma((5,)), dma((5,)), dma((steps,)), dma((steps,)),
                dma((4,)), dma((4,)), dma((5,)), dma((5,)), dma((steps,)),
            ],
            compiler_params=pltpu.CompilerParams(
                collective_id=0, has_side_effects=True, vmem_limit_bytes=60 * 1024 * 1024
            ),
            cost_estimate=pl.CostEstimate(flops=30_000_000_000, bytes_accessed=40_000_000, transcendentals=0),
        )(w_gate, w_up, w_down, x_norm, x_act.T, dy_gate, dy_up, dy_down, r_gate, c_gate, r_up, c_up, r_down, c_down, hyper_params)
        gg, gu, gd, wd_own, wd_near, dyd_all, own, rcg, rcu, rcd, rrow, crow, scal = outs
        pairs = [(0, 1), (1, 0)]
        early = [(k, (k + 4) % 8) for k in range(8) if k % 2 != LATE]
        wd_far = lax.ppermute(wd_own, ('col', 'row'), early)
        other = lax.ppermute(own, 'col', pairs)

        count = tokens // CHUNK
        grad_scratch = [vm((2, m2, n2), BF16), vm((2, tokens, n2), BF16), vm((m2, tokens), BF16)]
        grad_sems = [dma((2,)), dma((count,)), dma((count,))]
        dx_types = [sds((m2, tokens), BF16), sds((tokens, m1), BF16)]
        new_gate, new_up, new_down, dx_act, dx_norm, rg, cg, ru, cu, rd, cd = pl.pallas_call(
            update_kernel,
            name="update",
            out_shape=[sds((m1, n1), F32), sds((m1, n1), F32), sds((m2, n2), F32)] + dx_types + [
                sds((m1,), F32), sds((n1,), F32), sds((m1,), F32), sds((n1,), F32), sds((m2,), F32), sds((n2,), F32),
            ],
            in_specs=[any_spec] * 16,
            out_specs=[any_spec] * 11,
            scratch_shapes=[
                vm((m1, n1), F32), vm((m1, n1), F32), vm((m2, n2), F32),
                vm((m1, n1), F32), vm((m1, n1), F32), vm((m2, n2), F32),
                vm((m1, 128), F32), vm((m1, 128), F32), vm((m2, 128), F32),
                vm((8, 768), F32), vm((8, n1), F32), vm((8, 128), F32), vm((half, m1), BF16), *grad_scratch,
                vm((m1,), F32), vm((n1,), F32), vm((m1,), F32), vm((n1,), F32), vm((m2,), F32), vm((n2,), F32),
                dma((13,)), dma((10,)), *grad_sems,
            ],
            compiler_params=pltpu.CompilerParams(vmem_limit_bytes=VMEM_PLAIN),
            cost_estimate=pl.CostEstimate(flops=3_000_000_000, bytes_accessed=22_000_000, transcendentals=0),
        )(gg, gu, gd, w_gate, w_up, w_down, rcg, rcu, rcd, rrow, crow, scal, own, wd_own, wd_near, dyd_all)

        dx_act, dx_norm = pl.pallas_call(
            input_grad_kernel,
            name="input_grad",
            out_shape=dx_types,
            in_specs=[any_spec] * 5,
            out_specs=[any_spec] * 2,
            scratch_shapes=grad_scratch + grad_sems,
            input_output_aliases={3: 0, 4: 1},
            compiler_params=pltpu.CompilerParams(vmem_limit_bytes=VMEM_PLAIN),
            cost_estimate=pl.CostEstimate(flops=4 * tokens * m2 * n2, bytes_accessed=9_000_000, transcendentals=0),
        )(wd_own, wd_far, dyd_all, dx_act, dx_norm)

        start = (1 - lax.axis_index('col')) * half
        dx_norm = lax.dynamic_update_slice(dx_norm, other, (start, 0))
        return (new_gate, new_up, new_down, rg, cg, ru, cu, rd, cd, dx_norm, dx_act.T)

    return jax.shard_map(body, mesh=mesh, in_specs=in_specs, out_specs=out_specs, check_vma=False)
```

```python
import jax
import jax.numpy as jnp
from jax import lax
from jax.experimental import pallas as pl
from jax.experimental.pallas import tpu as pltpu
from jax.sharding import PartitionSpec as P

EPS_ONE = 1e-30
EPS_TWO = 1e-3
MESH = pl.DeviceIdType.MESH
F32 = jnp.float32
BF16 = jnp.bfloat16
NT = (((1,), (1,)), ((), ()))
CHUNK = 256
LATE = 1
EARLY_SIXTEENTHS = 4
VMEM_PLAIN = 65536 * 1024 - 700 * 1024


def dot(a, b, dims=(((1,), (0,)), ((), ()))):
    return lax.dot_general(a, b, dims, preferred_element_type=F32)


def to_row(column):
    return jnp.transpose(jnp.broadcast_to(column, (column.shape[0], 128)))[0:1, :]


def to_columns(row):
    return jnp.transpose(jnp.broadcast_to(row, (128, row.shape[1])))


def exchange_kernel(
    wg, wu, wd, xn, xat, dyg, dyu, dyd, rg, cg, ru, cu, rd, cd, hyper,
    gg_o, gu_o, gd_o, wd_o, wd_far, dyd_o, half_o, rcg_o, rcu_o, rcd_o, rrow_o, crow_o, scal_o,
    wg_v, wu_v, wd_v, wgb, wub, wdb, dyg_v, dyu_v, dyd_v, xn_v, xnt, xat_v, g_g, g_u, g_d,
    p_send, p_recv, p_own, half_v, rs_send, rs_recv, cs_send, cs_recv, s2_send, s2_recv, tot_send, tot_recv,
    rg_v, cg_v, ru_v, cu_v, rd_v, cd_v, rcg_v, rcu_v, rcd_v, rrow_v, crow_v, scal_v, b_v, hp,
    in_sem, out_sem, bulk_send, bulk_recv, p_ssem, p_rsem, st_send, st_recv, s2_ssem, s2_rsem, half_sem, dyd_sem,
):
    c = lax.axis_index("col")
    r = lax.axis_index("row")
    rows = {0: r, 1: r + 1 - 2 * (r % 2), 2: (r + 2) % 4, 3: 3 - r}
    cols = {0: c, 1: 1 - c}
    peers = [(1, 0), (0, 1), (0, 2), (0, 3)]

    def peer(a, b):
        return (cols[a], rows[b])

    def remote(src, dst, ssem, rsem, who):
        return pltpu.make_async_remote_copy(
            src_ref=src, dst_ref=dst, send_sem=ssem, recv_sem=rsem, device_id=who, device_id_type=MESH
        )

    tokens = dyg.shape[0]
    half = tokens // 2
    steps = half // CHUNK
    mine, theirs = pl.multiple_of(c * half, half), pl.multiple_of((1 - c) * half, half)

    few = half * EARLY_SIXTEENTHS // 16

    def part(x, core):
        start, size = (few, half - few) if core == LATE else (0, few)
        return pl.ds(pl.multiple_of(x * half + start, 64), size)

    def f1(core):
        at = part(r // 2, core)
        return remote(dyd_v.at[at], dyd_o.at[c, at], bulk_send.at[0], bulk_recv.at[0], peer(1, 0))

    def share(x, core, slot, who):
        at = part(x, core)
        return remote(dyd_o.at[1 - c, at], dyd_o.at[1 - c, at], bulk_send.at[slot], bulk_recv.at[slot], who)

    def on_core(body):
        for core in (0, 1):
            pl.when(r % 2 == core)(lambda core=core: body(core))

    near_x, far_x = r // 2, 1 - r // 2

    def dyd_load(core, slot):
        at = part(near_x, core)
        return pltpu.make_async_copy(dyd.at[at], dyd_v.at[at], dyd_sem.at[slot])

    on_core(lambda core: dyd_load(core, 0).start())

    barrier = pltpu.get_barrier_semaphore()
    for a, b in peers:
        pl.semaphore_signal(barrier, inc=1, device_id=peer(a, b), device_id_type=MESH)

    loads = []

    def load(src, dst):
        copy = pltpu.make_async_copy(src, dst, in_sem.at[len(loads)])
        copy.start()
        loads.append(copy)
        return copy

    l_wg = load(wg, wg_v)
    l_wu = load(wu, wu_v)
    l_dg1 = load(dyg.at[pl.ds(theirs, half)], dyg_v.at[pl.ds(theirs, half)])
    l_du1 = load(dyu.at[pl.ds(theirs, half)], dyu_v.at[pl.ds(theirs, half)])
    l_xn = load(xn, xn_v)
    l_dg2 = load(dyg.at[pl.ds(mine, half)], dyg_v.at[pl.ds(mine, half)])
    l_du2 = load(dyu.at[pl.ds(mine, half)], dyu_v.at[pl.ds(mine, half)])
    l_xat = load(xat, xat_v)
    far_rows = pl.ds(pl.multiple_of(far_x * half, half), half)
    l_dyd = load(dyd.at[far_rows], dyd_v.at[far_rows])
    on_core(lambda core: dyd_load(1 - core, 1).start())
    l_wd = load(wd, wd_v)
    l_small = [load(src, dst) for src, dst in ((rg, rg_v), (cg, cg_v), (ru, ru_v), (cu, cu_v), (rd, rd_v), (cd, cd_v), (hyper, hp))]

    pl.semaphore_wait(barrier, len(peers))

    @on_core
    def _(core):
        dyd_load(core, 0).wait()
        f1(core).start()

    outs = []

    def store(src, dst):
        copy = pltpu.make_async_copy(src, dst, out_sem.at[len(outs)])
        copy.start()
        outs.append(copy)

    l_wg.wait()
    wgb[...] = wg_v[...].astype(BF16)
    l_wu.wait()
    wub[...] = wu_v[...].astype(BF16)
    l_dg1.wait()
    l_du1.wait()

    def p_copy(i):
        rows_i = pl.ds(pl.multiple_of(i * CHUNK, CHUNK), CHUNK)
        return remote(p_send.at[rows_i], p_recv.at[rows_i], p_ssem.at[i], p_rsem.at[i], peer(1, 0))

    def partial(base, i):
        rows_i = pl.ds(pl.multiple_of(base + i * CHUNK, CHUNK), CHUNK)
        return dot(dyg_v[rows_i, :], wgb[...], NT) + dot(dyu_v[rows_i, :], wub[...], NT)

    @pl.loop(0, steps // 2)
    def _(i):
        p_send[pl.ds(pl.multiple_of(i * CHUNK, CHUNK), CHUNK), :] = partial(theirs, i)
        pl.when(r % 2 != LATE)(lambda: p_copy(i).start())

    @pl.loop(steps // 2, steps)
    def _(i):
        p_send[pl.ds(pl.multiple_of(i * CHUNK, CHUNK), CHUNK), :] = partial(theirs, i)

    (m1, n1) = g_g.shape
    row_offsets, col_offsets = (0, m1, 2 * m1), (0, n1, 2 * n1)
    rs_send[...] = jnp.zeros_like(rs_send)
    l_xn.wait()

    @pl.loop(0, tokens // 256)
    def _(i):
        at = pl.ds(pl.multiple_of(i * 256, 256), 256)
        xnt[:, at] = jnp.transpose(xn_v[at, :])

    l_dg2.wait()
    l_du2.wait()

    def gradient(index, lhs, rhs, out):
        m, n = out.shape
        row_at, col_at = row_offsets[index], col_offsets[index]

        def block(lo, width, acc):
            at = pl.ds(lo, width)
            g = dot(lhs[...], rhs[:, at])
            out[:, at] = g
            sq = g * g + EPS_ONE
            cs_send[:, pl.ds(col_at + lo, width)] = jnp.sum(sq, axis=0, keepdims=True)
            for part in range(0, width, 128):
                acc = acc + sq[:, part:part + 128]
            return acc

        full = n // 256
        acc = lax.fori_loop(
            0, full, lambda i, acc: block(pl.multiple_of(i * 256, 256), 256, acc), jnp.zeros((m, 128), F32))
        if n % 256:
            acc = block(full * 256, n % 256, acc)
        rs_send[:, row_at:row_at + m] = to_row(jnp.sum(acc, axis=1, keepdims=True))

    gradient(0, xnt, dyg_v, g_g)
    gradient(1, xnt, dyu_v, g_u)
    l_xat.wait()
    l_dyd.wait()
    on_core(lambda core: dyd_load(1 - core, 1).wait())
    gradient(2, xat_v, dyd_v, g_d)

    s1_row = remote(rs_send, rs_recv, st_send.at[0], st_recv.at[0], peer(1, 0))
    s1_row.start()
    s1_col = []
    for b in (1, 2, 3):
        copy = remote(cs_send, cs_recv.at[b - 1], st_send.at[b], st_recv.at[b], peer(0, b))
        copy.start()
        s1_col.append(copy)

    @pl.when(r % 2 == LATE)
    def _():
        @pl.loop(0, steps // 2)
        def _(i):
            p_copy(i).start()

    @pl.loop(steps // 2, steps)
    def _(i):
        p_copy(i).start()

    store(g_g, gg_o)
    store(g_u, gu_o)
    store(g_d, gd_o)
    store(dyd_v, dyd_o.at[c])

    l_wd.wait()
    wdb[...] = wd_v[...].astype(BF16)
    store(wdb, wd_o)
    f3 = remote(wdb, wd_far, bulk_send.at[4], bulk_recv.at[4], peer(1, 0))

    @pl.when(r % 2 == LATE)
    def _():
        f3.start()


    w_sq = [jnp.sum(jnp.sum(w[...] * w[...], axis=0, keepdims=True), axis=1, keepdims=True) for w in (wg_v, wu_v, wd_v)]

    @pl.loop(0, steps)
    def _(i):
        p_own[pl.ds(pl.multiple_of(i * CHUNK, CHUNK), CHUNK), :] = partial(mine, i)

    @on_core
    def _(core):
        f1(core).wait()
        share(near_x, core, 1, peer(0, 1)).start()
        share(near_x, core, 2, peer(0, 2)).start()

    s1_row.wait_recv()
    for copy in s1_col:
        copy.wait_recv()
    for copy in l_small:
        copy.wait()
    beta = hp[0]
    shapes = [g.shape for g in (g_g, g_u, g_d)]
    qs, ss = [], []
    rrow_v[...] = jnp.zeros_like(rrow_v)
    crow_v[...] = jnp.ones_like(crow_v)
    for index, (g, r_ref, c_ref, rc_v) in enumerate(((g_g, rg_v, cg_v, rcg_v), (g_u, ru_v, cu_v, rcu_v), (g_d, rd_v, cd_v, rcd_v))):
        m, n = shapes[index]
        m_all, n_all = m * 4, n * 2
        row_at, col_at = pl.ds(row_offsets[index], m), pl.ds(col_offsets[index], n)
        row_sum = rs_send[:, row_at] + rs_recv[:, row_at]
        col_sum = (cs_send[:, col_at] + cs_recv[0, :, col_at]) + (cs_recv[1, :, col_at] + cs_recv[2, :, col_at])
        r_new = beta * r_ref[...].reshape(1, m) + (1.0 - beta) * (row_sum / n_all)
        c_new = beta * c_ref[...].reshape(1, n) + (1.0 - beta) * (col_sum / m_all)
        rrow_v[index:index + 1, 0:m] = r_new
        crow_v[index:index + 1, 0:n] = c_new
        q = jnp.sum(r_new, axis=1, keepdims=True) / m_all
        columns = to_columns(r_new)
        rc_v[...] = columns
        a = lax.rsqrt(columns / q)
        b_v[:, 0:n] = lax.rsqrt(c_new)

        def square(i, acc, g=g, a=a):
            at = pl.ds(pl.multiple_of(i * 128, 128), 128)
            u = g[:, at] * (a * b_v[:, at])
            return acc + u * u

        acc = lax.fori_loop(0, n // 128, square, jnp.zeros((m, 128), F32))
        qs.append(q)
        ss.append(jnp.sum(jnp.sum(acc, axis=0, keepdims=True), axis=1, keepdims=True))

    lane = lax.broadcasted_iota(jnp.int32, (1, 128), 1)

    def lanes(values, fill):
        out = jnp.full((1, 128), fill, F32)
        for index, value in enumerate(values):
            out = jnp.where(lane == index, value, out)
        return out

    s2_send[:, 0:128] = lanes(qs, 1.0)
    s2_send[:, 128:256] = lanes(ss, 0.0)
    s2_send[:, 256:384] = lanes(w_sq, 0.0)
    s2 = []
    for b in (1, 2, 3):
        copy = remote(s2_send, s2_recv.at[b - 1], s2_ssem.at[b - 1], s2_rsem.at[b - 1], peer(0, b))
        copy.start()
        s2.append(copy)

    for src, dst in ((rcg_v, rcg_o), (rcu_v, rcu_o), (rcd_v, rcd_o), (rrow_v, rrow_o), (crow_v, crow_o)):
        store(src, dst)

    def half_copy(i):
        rows_i = pl.ds(pl.multiple_of(i * CHUNK, CHUNK), CHUNK)
        return pltpu.make_async_copy(half_v.at[rows_i], half_o.at[rows_i], half_sem.at[i])

    @on_core
    def _(core):
        share(far_x, core, 2, peer(0, 2)).wait_recv()
        share(far_x, core, 3, peer(0, 1)).start()

    for copy in s2:
        copy.wait_recv()
    table = [s2_send[...]] + [s2_recv[k] for k in range(3)]

    def tree(values):
        return (values[0] + values[1]) + (values[2] + values[3])

    r_mean = tree([t[:, 0:128] for t in table])
    u_sq = []
    for t in table:
        ratio = jnp.sqrt(r_mean) / jnp.sqrt(t[:, 0:128])
        u_sq.append((t[:, 128:256] * ratio) * ratio)
    tot_send[:, 0:128] = tree(u_sq)
    tot_send[:, 128:256] = tree([t[:, 256:384] for t in table])

    tot_copy = remote(tot_send, tot_recv, s2_ssem.at[3], s2_rsem.at[3], peer(1, 0))
    tot_tell = remote(tot_recv, tot_recv, s2_ssem.at[4], s2_rsem.at[4], peer(0, 1))

    @pl.when(r % 2 != LATE)
    def _():
        tot_copy.start()

    @pl.loop(0, steps)
    def _(i):
        rows_i = pl.ds(pl.multiple_of(i * CHUNK, CHUNK), CHUNK)
        p_copy(i).wait_recv()
        half_v[rows_i, :] = (p_own[rows_i, :] + p_recv[rows_i, :]).astype(BF16)
        half_copy(i).start()

    @pl.when(r % 2 != LATE)
    def _():
        tot_copy.wait()
        tot_tell.start()

    @pl.when(r % 2 == LATE)
    def _():
        tot_tell.wait_recv()

    total = tot_send[...] + tot_recv[...]
    size = F32(shapes[0][0] * shapes[0][1] * 8)
    rms_u = jnp.sqrt(total[:, 0:128] / size)
    step_size = hp[1] * jnp.maximum(EPS_TWO, jnp.sqrt(total[:, 128:256] / size))
    scal_v[...] = jnp.zeros_like(scal_v)
    scal_v[0:1, :] = r_mean
    scal_v[1:2, :] = 1.0 / jnp.maximum(1.0, rms_u / hp[2])
    scal_v[2:3, :] = step_size
    store(scal_v, scal_o)


    @on_core
    def _(core):
        share(near_x, 1 - core, 1, peer(0, 1)).wait_recv()
        share(far_x, 1 - core, 3, peer(0, 1)).wait_recv()
        share(near_x, core, 1, peer(0, 1)).wait_send()
        share(near_x, core, 2, peer(0, 2)).wait_send()
        share(far_x, core, 3, peer(0, 1)).wait_send()

    @pl.when(r % 2 == LATE)
    def _():
        f3.wait()

    @pl.when(r % 2 != LATE)
    def _():
        tot_tell.wait_send()

    for copy in [s1_row] + s1_col + s2:
        copy.wait_send()

    @pl.loop(0, steps)
    def _(i):
        p_copy(i).wait_send()
        half_copy(i).wait()

    for copy in outs:
        copy.wait()


def token_rows(i):
    return pl.ds(pl.multiple_of(i * CHUNK, CHUNK), CHUNK)


class InputGrad:
    def __init__(self, wd_own, wd_other, dyd_all, dx_o, wd_all, dyd_v, dx_v, wd_sem, dyd_sem, dx_sem):
        c = lax.axis_index("col")
        self.count = dyd_v.shape[1] // CHUNK
        self.weights = [
            pltpu.make_async_copy(wd_own, wd_all.at[c], wd_sem.at[0]),
            pltpu.make_async_copy(wd_other, wd_all.at[1 - c], wd_sem.at[1]),
        ]
        self.refs = wd_all, dyd_all, dyd_v, dx_v, dx_o, dyd_sem, dx_sem

    def dyd_copy(self, i):
        wd_all, dyd_all, dyd_v, dx_v, dx_o, dyd_sem, dx_sem = self.refs
        return pltpu.make_async_copy(dyd_all.at[:, token_rows(i)], dyd_v.at[:, token_rows(i)], dyd_sem.at[i])

    def dx_copy(self, i):
        wd_all, dyd_all, dyd_v, dx_v, dx_o, dyd_sem, dx_sem = self.refs
        return pltpu.make_async_copy(dx_v.at[:, token_rows(i)], dx_o.at[:, token_rows(i)], dx_sem.at[i])

    def fetch(self, lo, hi):
        @pl.loop(lo, hi)
        def _(i):
            self.dyd_copy(i).start()

    def multiply(self, lo, hi):
        wd_all, dyd_all, dyd_v, dx_v, dx_o, dyd_sem, dx_sem = self.refs

        @pl.loop(lo, hi)
        def _(i):
            self.dyd_copy(i).wait()
            dx = dot(wd_all[0], dyd_v[0, token_rows(i), :], NT) + dot(wd_all[1], dyd_v[1, token_rows(i), :], NT)
            dx_v[:, token_rows(i)] = dx.astype(BF16)
            self.dx_copy(i).start()

    def finish(self):
        @pl.loop(0, self.count)
        def _(i):
            self.dx_copy(i).wait()


def update_kernel(
    gg, gu, gd, wg, wu, wd, rcg, rcu, rcd, rrow, crow, scal, own, wd_own, wd_near, dyd_all,
    wg_o, wu_o, wd_o, dx_o, dxn_o, rg_o, cg_o, ru_o, cu_o, rd_o, cd_o,
    gg_v, gu_v, gd_v, wg_v, wu_v, wd_v, rcg_v, rcu_v, rcd_v, rrow_v, crow_v, scal_v, own_v, wd_all, dyd_v, dx_v,
    rg_v, cg_v, ru_v, cu_v, rd_v, cd_v, in_sem, out_sem, wd_sem, dyd_sem, dx_sem,
):
    c = lax.axis_index("col")
    late = lax.axis_index("row") % 2 == LATE
    half = own.shape[0]
    grad = InputGrad(wd_own, wd_near, dyd_all, dx_o, wd_all, dyd_v, dx_v, wd_sem, dyd_sem, dx_sem)
    loads, outs = [], []

    def load(src, dst):
        copy = pltpu.make_async_copy(src, dst, in_sem.at[len(loads)])
        loads.append(copy)
        copy.start()
        return copy

    def store(src, dst):
        copy = pltpu.make_async_copy(src, dst, out_sem.at[len(outs)])
        outs.append(copy)
        copy.start()

    l_gg, l_wg = load(gg, gg_v), load(wg, wg_v)
    l_small = [load(rcg, rcg_v), load(rcu, rcu_v), load(rcd, rcd_v), load(rrow, rrow_v), load(crow, crow_v), load(scal, scal_v)]

    @pl.when(late)
    def _():
        for copy in grad.weights:
            copy.start()
        grad.fetch(0, 3)

    l_gu, l_wu = load(gu, gu_v), load(wu, wu_v)

    @pl.when(late)
    def _():
        grad.fetch(3, 6)

    l_gd, l_wd = load(gd, gd_v), load(wd, wd_v)
    l_own = load(own, own_v)

    @pl.when(late)
    def _():
        grad.fetch(6, grad.count)

    def update(index, waits, g, w, rc, out):
        for copy in waits:
            copy.wait()
        n = g.shape[1]
        r_mean = scal_v[0:1, index:index + 1]
        inv = scal_v[1:2, index:index + 1]
        step = scal_v[2:3, index:index + 1]
        a = lax.rsqrt(rc[...] / r_mean)
        b_row = lax.rsqrt(crow_v[index:index + 1, 0:n])
        for lo in range(0, n, 128):
            u = g[:, lo:lo + 128] * (a * b_row[:, lo:lo + 128])
            w[:, lo:lo + 128] = w[:, lo:lo + 128] - step * (u * inv)
        store(w, out)

    for copy in l_small:
        copy.wait()
    update(0, (l_gg, l_wg), gg_v, wg_v, rcg_v, wg_o)
    for index, (r_v, c_v, r_out, c_out) in enumerate(
            ((rg_v, cg_v, rg_o, cg_o), (ru_v, cu_v, ru_o, cu_o), (rd_v, cd_v, rd_o, cd_o))):
        r_v[...] = rrow_v[index:index + 1, 0:r_v.shape[0]].reshape(r_v.shape)
        c_v[...] = crow_v[index:index + 1, 0:c_v.shape[0]].reshape(c_v.shape)
        store(r_v, r_out)
        store(c_v, c_out)

    @pl.when(late)
    def _():
        for copy in grad.weights:
            copy.wait()
        grad.multiply(0, 3)

    update(1, (l_gu, l_wu), gu_v, wu_v, rcu_v, wu_o)

    @pl.when(late)
    def _():
        grad.multiply(3, 6)

    update(2, (l_gd, l_wd), gd_v, wd_v, rcd_v, wd_o)
    l_own.wait()
    store(own_v, dxn_o.at[pl.ds(pl.multiple_of(c * half, half), half)])

    @pl.when(late)
    def _():
        grad.multiply(6, grad.count)
        grad.finish()

    for copy in outs:
        copy.wait()


def input_grad_kernel(
    wd_own, wd_far, dyd_all, dx_in, dxn_in, dx_o, dxn_o, wd_all, dyd_v, dx_v, wd_sem, dyd_sem, dx_sem,
):
    grad = InputGrad(wd_own, wd_far, dyd_all, dx_o, wd_all, dyd_v, dx_v, wd_sem, dyd_sem, dx_sem)

    @pl.when(lax.axis_index("row") % 2 != LATE)
    def _():
        grad.fetch(0, 1)
        for copy in grad.weights:
            copy.start()
        grad.fetch(1, grad.count)
        for copy in grad.weights:
            copy.wait()
        grad.multiply(0, grad.count)
        grad.finish()


def solution(mesh):
    weight_spec = P('row', 'col')
    act_spec = P(None, 'row')
    grad_spec = P(None, 'col')
    in_specs = (weight_spec,) * 3 + (act_spec, act_spec) + (grad_spec,) * 3 + (P('row'), P('col')) * 3 + (P(),)
    out_specs = (weight_spec,) * 3 + (P('row'), P('col')) * 3 + (act_spec, act_spec)

    def body(w_gate, w_up, w_down, x_norm, x_act, dy_gate, dy_up, dy_down, r_gate, c_gate, r_up, c_up, r_down, c_down, hyper_params):
        m1, n1 = w_gate.shape
        m2, n2 = w_down.shape
        tokens = x_norm.shape[0]
        half = tokens // 2
        steps = half // CHUNK
        row_len, col_len = 2 * m1 + 768, 2 * n1 + n2
        any_spec = pl.BlockSpec(memory_space=pl.ANY)
        sds = jax.ShapeDtypeStruct
        vm = pltpu.VMEM
        dma = pltpu.SemaphoreType.DMA
        outs = pl.pallas_call(
            exchange_kernel,
            name="exchange",
            out_shape=[
                sds((m1, n1), F32), sds((m1, n1), F32), sds((m2, n2), F32),
                sds((m2, n2), BF16), sds((m2, n2), BF16), sds((2, tokens, n2), BF16), sds((half, m1), BF16),
                sds((m1, 128), F32), sds((m1, 128), F32), sds((m2, 128), F32),
                sds((8, 768), F32), sds((8, n1), F32), sds((8, 128), F32),
            ],
            in_specs=[any_spec] * 15,
            out_specs=[any_spec] * 13,
            scratch_shapes=[
                vm((m1, n1), F32), vm((m1, n1), F32), vm((m2, n2), F32),
                vm((m1, n1), BF16), vm((m1, n1), BF16), vm((m2, n2), BF16),
                vm((tokens, n1), BF16), vm((tokens, n1), BF16), vm((tokens, n2), BF16),
                vm((tokens, m1), BF16), vm((m1, tokens), BF16), vm((m2, tokens), BF16),
                vm((m1, n1), F32), vm((m1, n1), F32), vm((m2, n2), F32),
                vm((half, m1), F32), vm((half, m1), F32), vm((half, m1), F32), vm((half, m1), BF16),
                vm((1, row_len), F32), vm((1, row_len), F32), vm((1, col_len), F32), vm((3, 1, col_len), F32),
                vm((1, 384), F32), vm((3, 1, 384), F32), vm((1, 256), F32), vm((1, 256), F32),
                vm((m1,), F32), vm((n1,), F32), vm((m1,), F32), vm((n1,), F32), vm((m2,), F32), vm((n2,), F32),
                vm((m1, 128), F32), vm((m1, 128), F32), vm((m2, 128), F32),
                vm((8, 768), F32), vm((8, n1), F32), vm((8, 128), F32), vm((1, n1), F32), pltpu.SMEM((3,), F32),
                dma((17,)), dma((12,)), dma((5,)), dma((5,)), dma((steps,)), dma((steps,)),
                dma((4,)), dma((4,)), dma((5,)), dma((5,)), dma((steps,)), dma((2,)),
            ],
            compiler_params=pltpu.CompilerParams(
                collective_id=0, has_side_effects=True, vmem_limit_bytes=60 * 1024 * 1024
            ),
            cost_estimate=pl.CostEstimate(flops=30_000_000_000, bytes_accessed=40_000_000, transcendentals=0),
        )(w_gate, w_up, w_down, x_norm, x_act.T, dy_gate, dy_up, dy_down, r_gate, c_gate, r_up, c_up, r_down, c_down, hyper_params)
        gg, gu, gd, wd_own, wd_near, dyd_all, own, rcg, rcu, rcd, rrow, crow, scal = outs
        pairs = [(0, 1), (1, 0)]
        early = [(k, (k + 4) % 8) for k in range(8) if k % 2 != LATE]
        wd_far = lax.ppermute(wd_own, ('col', 'row'), early)
        other = lax.ppermute(own, 'col', pairs)

        count = tokens // CHUNK
        grad_scratch = [vm((2, m2, n2), BF16), vm((2, tokens, n2), BF16), vm((m2, tokens), BF16)]
        grad_sems = [dma((2,)), dma((count,)), dma((count,))]
        dx_types = [sds((m2, tokens), BF16), sds((tokens, m1), BF16)]
        new_gate, new_up, new_down, dx_act, dx_norm, rg, cg, ru, cu, rd, cd = pl.pallas_call(
            update_kernel,
            name="update",
            out_shape=[sds((m1, n1), F32), sds((m1, n1), F32), sds((m2, n2), F32)] + dx_types + [
                sds((m1,), F32), sds((n1,), F32), sds((m1,), F32), sds((n1,), F32), sds((m2,), F32), sds((n2,), F32),
            ],
            in_specs=[any_spec] * 16,
            out_specs=[any_spec] * 11,
            scratch_shapes=[
                vm((m1, n1), F32), vm((m1, n1), F32), vm((m2, n2), F32),
                vm((m1, n1), F32), vm((m1, n1), F32), vm((m2, n2), F32),
                vm((m1, 128), F32), vm((m1, 128), F32), vm((m2, 128), F32),
                vm((8, 768), F32), vm((8, n1), F32), vm((8, 128), F32), vm((half, m1), BF16), *grad_scratch,
                vm((m1,), F32), vm((n1,), F32), vm((m1,), F32), vm((n1,), F32), vm((m2,), F32), vm((n2,), F32),
                dma((13,)), dma((10,)), *grad_sems,
            ],
            compiler_params=pltpu.CompilerParams(vmem_limit_bytes=VMEM_PLAIN),
            cost_estimate=pl.CostEstimate(flops=3_000_000_000, bytes_accessed=22_000_000, transcendentals=0),
        )(gg, gu, gd, w_gate, w_up, w_down, rcg, rcu, rcd, rrow, crow, scal, own, wd_own, wd_near, dyd_all)

        dx_act, dx_norm = pl.pallas_call(
            input_grad_kernel,
            name="input_grad",
            out_shape=dx_types,
            in_specs=[any_spec] * 5,
            out_specs=[any_spec] * 2,
            scratch_shapes=grad_scratch + grad_sems,
            input_output_aliases={3: 0, 4: 1},
            compiler_params=pltpu.CompilerParams(vmem_limit_bytes=VMEM_PLAIN),
            cost_estimate=pl.CostEstimate(flops=4 * tokens * m2 * n2, bytes_accessed=9_000_000, transcendentals=0),
        )(wd_own, wd_far, dyd_all, dx_act, dx_norm)

        start = (1 - lax.axis_index('col')) * half
        dx_norm = lax.dynamic_update_slice(dx_norm, other, (start, 0))
        return (new_gate, new_up, new_down, rg, cg, ru, cu, rd, cd, dx_norm, dx_act.T)

    return jax.shard_map(body, mesh=mesh, in_specs=in_specs, out_specs=out_specs, check_vma=False)
```
